512 devices in a mesh: samp: 128 (over z, y, core), snp: 4 (over x).
Axes of the slice: x: 4, y: 4, z: 16, core: 2. Of those that a mesh axis runs over, the one named last changes fastest.
Arguments:
- geno_words: int32 [32768, 1024], P('samp', 'snp'), may hold values from -2147483648 to 2147483647, as said below
- counts: int32 [32768], P('samp'), may hold values from 0 to 4, as said below
- probes: bfloat16 [32768, 64], P('samp'), may hold values from -6 to 6
- phenotype: float32 [32768], P('samp'), may hold values from -6 to 6
- tile_comp: int32 [128], replicated, may hold values from 0 to 7, as said below
Outputs:
- images: bfloat16 [32768, 512], P(('samp', 'snp'))
- traces: float32 [8, 8], replicated
- yky: float32 [8], replicated
The draws below stay inside these ranges and needn't reach their ends.
Inputs may be any that keep to these rules, and one draw needn't show every extreme that they name: `geno_words`: each word packs sixteen dosages of one sample in 2-bit fields as step one reads them; every field holds 0, 1 or 2. `counts`: at least one sample has a count of one or more. `tile_comp`: every component owns at least one tile.
All inputs are finite; a program needn't handle non-finite values.
Results may differ from the reference program's by a relative error of at most 0.015.
Values may be sent and summed in bfloat16 or wider, within the bound.
No kernel may reach another device: no remote copies, remote signals or barrier semaphores. Data moves between devices by JAX's collectives and lax.ppermute only.
A program may use at most 64 MiB of HBM per device.

```python
import math
import jax
import jax.numpy as jnp
from jax import lax

SNPS = 16384
PROBES = 64
COMPS = 8
NS = 32768
TILES = 128


def draw_geno_words(key, part):
    base = jax.random.randint(jax.random.fold_in(key, 11), (SNPS,), 51, 165)
    stride = math.gcd(NS, 512)
    shifts = 2 * jnp.arange(16, dtype=jnp.int32).reshape(1, 1, 16, 1)
    block_key = jax.random.fold_in(key, 12)

    def one_block(first_row):
        sample_ids = first_row + jnp.arange(stride, dtype=jnp.int32)
        levels = base[None, :] * (NS + 2 * sample_ids[:, None]) // NS
        drawn = jax.random.randint(jax.random.fold_in(block_key, first_row), (stride, SNPS), 0, 1048576)
        dosage = (drawn % 1024 < levels).astype(jnp.int32) + (drawn // 1024 < levels).astype(jnp.int32)
        fields = jnp.left_shift(dosage.reshape(stride, SNPS // 2048, 16, 128), shifts)
        return jnp.sum(fields, axis=2).reshape(stride, SNPS // 16)
    starts = jnp.arange(NS // stride, dtype=jnp.int32) * stride
    return lax.map(one_block, starts).reshape(NS, SNPS // 16)


def draw_counts(key, part):
    drawn = jax.random.randint(jax.random.fold_in(key, 21), (NS,), 0, 5)
    chosen = jax.random.randint(jax.random.fold_in(key, 22), (), 0, NS)
    return drawn.at[chosen].set(jnp.maximum(drawn[chosen], 1))


def draw_tile_comp(key, part):
    drawn = jax.random.randint(jax.random.fold_in(key, 31), (TILES,), 0, COMPS)
    shuffled = jax.random.permutation(jax.random.fold_in(key, 32), TILES)
    return drawn.at[shuffled[:COMPS]].set(jnp.arange(COMPS, dtype=jnp.int32))


def steps_of(own_key, extent, pieces, low, largest):
    gain, own = 1.0, jax.random.fold_in(own_key, 6)
    for position, shards_of in pieces:
        heights = jnp.exp(jax.random.uniform(jax.random.fold_in(own, position), (shards_of,), jnp.float32, low / len(pieces), largest / len(pieces)))
        gain = gain * jnp.repeat(heights, extent[position] // shards_of).reshape([-1 if axis == position else 1 for axis in range(len(extent))])
    return gain


def gaussian(key, extent, width, bound, pieces=(), held_as=jnp.bfloat16):
    values = width * jax.random.normal(key, extent, jnp.float32)
    if pieces:
        values = values * steps_of(key, extent, pieces, -0.22, 0.18)
    return jnp.clip(values, -bound, bound).astype(held_as)


def setup_inputs(seed: int = 0) -> dict:
    splits = jax.random.split(jax.random.key(seed), 6)
    return {
        "geno_words": draw_geno_words(jax.random.fold_in(splits[5], 71), 0),
        "counts": draw_counts(jax.random.fold_in(splits[5], 71), 0),
        "probes": gaussian(splits[2], (NS, PROBES), 1.0, 6.0, ((0, 128),)),
        "phenotype": gaussian(splits[3], (NS,), 1.0, 6.0, ((0, 128),), jnp.float32),
        "tile_comp": draw_tile_comp(jax.random.fold_in(splits[5], 71), 0),
    }


EPSILON = 1e-05

def unpack_rows(packed):
    height = packed.shape[0]
    grouped = packed.reshape(height, -1, 1, 128)
    shifts = 2 * jnp.arange(16, dtype=jnp.int32).reshape(1, 1, 16, 1)
    fields = jnp.right_shift(grouped, shifts) & 3
    return fields.reshape(height, -1).astype(jnp.bfloat16)

def reference(geno_words, counts, probes, phenotype, tile_comp):
    weights = counts.astype(jnp.float32)
    root_weight = jnp.sqrt(weights)
    probe_rows = (probes.astype(jnp.float32) * root_weight[:, None]).astype(jnp.bfloat16)
    pheno_rows = (phenotype * root_weight).astype(jnp.bfloat16)
    count_rows = counts.astype(jnp.bfloat16)
    stride = math.gcd(NS, 1024)
    blocks = NS // stride
    packed_blocks = geno_words.reshape(blocks, stride, SNPS // 16)

    def first_pass(running, inputs):
        cross_panel, moments = running
        packed, probe_block, pheno_block, count_block = inputs
        dosage = unpack_rows(packed)
        cross_panel = cross_panel + jnp.dot(dosage.T, probe_block, preferred_element_type=jnp.float32)
        increment = jnp.stack([jnp.dot(count_block, dosage, preferred_element_type=jnp.float32), jnp.dot(count_block, dosage * dosage, preferred_element_type=jnp.float32), jnp.dot(pheno_block, dosage, preferred_element_type=jnp.float32)])
        return ((cross_panel, moments + increment), None)
    start_pair = (jnp.zeros((SNPS, PROBES), jnp.float32), jnp.zeros((3, SNPS), jnp.float32))
    (cross_panel, moments), ignored = lax.scan(first_pass, start_pair, (packed_blocks, probe_rows.reshape(blocks, stride, PROBES), pheno_rows.reshape(blocks, stride), count_rows.reshape(blocks, stride)))
    weight_total = jnp.sum(weights)
    pheno_total = jnp.sum(pheno_rows.astype(jnp.float32))
    probe_total = lax.optimization_barrier(jnp.sum(probe_rows.astype(jnp.float32), axis=0))
    average = moments[0] / weight_total
    second = moments[1] / weight_total
    spread = 1.0 / jnp.sqrt(second - average * average + EPSILON)
    unit_panel = spread[:, None] * (cross_panel - average[:, None] * probe_total[None, :])
    pheno_unit = spread * (moments[2] - average * pheno_total)
    levels = jnp.arange(COMPS, dtype=jnp.int32)
    member_tiles = (tile_comp[:, None] == levels[None, :]).astype(jnp.float32)
    comp_sizes = 128.0 * lax.optimization_barrier(jnp.sum(member_tiles, axis=0))
    member_snps = jnp.repeat(member_tiles, 128, axis=0)
    inverse = lax.optimization_barrier(jnp.sum(member_snps * (1.0 / comp_sizes)[None, :], axis=1))
    coefficients = (spread[:, None] * unit_panel * inverse[:, None]).astype(jnp.bfloat16)
    energy = lax.optimization_barrier(jnp.sum(member_snps * (pheno_unit * pheno_unit * inverse)[:, None], axis=0))
    coef_tiles = coefficients.reshape(TILES, 128, PROBES).astype(jnp.float32)
    centre = lax.optimization_barrier(jnp.sum(average.reshape(TILES, 128, 1) * coef_tiles, axis=1))

    def second_pass(running, inputs):
        packed, root_block = inputs
        dosage = unpack_rows(packed).astype(jnp.float32).reshape(stride, TILES, 128)
        partial_value = jnp.einsum('rtj,tjb->rtb', dosage, coef_tiles, precision=lax.Precision.HIGHEST) - centre[None]
        grouped = jnp.einsum('rtb,tk->rkb', partial_value, member_tiles, precision=lax.Precision.HIGHEST)
        grouped = grouped * root_block[:, None, None]
        running = running + jnp.einsum('rkb,rlb->kl', grouped, grouped, precision=lax.Precision.HIGHEST)
        return (running, grouped.reshape(stride, COMPS * PROBES).astype(jnp.bfloat16))
    trace_sum, images = lax.scan(second_pass, jnp.zeros((COMPS, COMPS), jnp.float32), (packed_blocks, root_weight.reshape(blocks, stride)))
    traces = trace_sum * (SNPS / (COMPS * PROBES)) / (weight_total * weight_total)
    return (images.reshape(NS, COMPS * PROBES), traces, energy / weight_total)
```

```python
import jax
import jax.numpy as jnp
import numpy as np
from jax import lax
from jax.experimental import pallas as pl
from jax.experimental.pallas import tpu as pltpu
from jax.sharding import Mesh
from jax.sharding import PartitionSpec as P

SNPS = 16384
COMPS = 8
PROBES = 64
EPSILON = 1e-05
F32 = jnp.float32
BF16 = jnp.bfloat16

PHENO, FIRST, SQUARE, RATE, TOTALS = 64, 65, 67, 69, 70
COUNT = 65
ROWS = 72


def rounded(v):
    return v.astype(BF16).astype(F32)


def two_parts(v):
    high = rounded(v)
    return high, v - high


def three_parts(v):
    high = rounded(v)
    rest = v - high
    mid = rounded(rest)
    return high, mid, rest - mid


def stacked(rows, height):
    width = rows[0].shape[1]
    at = lax.broadcasted_iota(jnp.int32, (height, width), 0)
    out = jnp.zeros((height, width), F32)
    for i, row in enumerate(rows):
        out = jnp.where(at == i, jnp.broadcast_to(row, (height, width)), out)
    return out


def rate_of(weight):
    return rounded(1.0 / jnp.maximum(weight, 1.0))


def dot_tn(a, b):
    return lax.dot_general(a, b, (((0,), (0,)), ((), ())), preferred_element_type=F32)


def dot_nt(a, b):
    return lax.dot_general(a, b, (((1,), (1,)), ((), ())), preferred_element_type=F32)


def dosage_tile(words, tile):
    half, field = divmod(tile, 16)
    block = words[:, 128 * half : 128 * half + 128]
    return (lax.shift_right_logical(block, jnp.int32(2 * field)) & 3).astype(F32)


def panel_kernel(words_ref, probes_ref, counts_ref, pheno_ref, out_ref):
    counts = counts_ref[...].astype(F32)
    root = jnp.sqrt(counts)
    probes = probes_ref[...].astype(F32)
    wide = jnp.concatenate([probes, jnp.zeros_like(probes)], axis=1)
    probe_rows = (wide.T[:64] * root).astype(BF16).astype(F32)
    pheno_rows = rounded(pheno_ref[...] * root)
    tail = stacked([pheno_rows, counts], 64)
    left_all = jnp.concatenate([probe_rows, tail], axis=0)
    left = left_all[:ROWS].astype(BF16)
    left_tail = left_all[64:72].astype(BF16)
    totals = dot_nt(jnp.ones((8, left_all.shape[1]), BF16), left_all.astype(BF16))[:1]
    column = jnp.sum(left_all[:ROWS], axis=1, keepdims=True)
    rate = rate_of(jnp.sum(counts, axis=1, keepdims=True))
    parts = three_parts(totals)
    totals_row = jnp.concatenate([*parts, jnp.zeros_like(totals)], axis=1)
    words = words_ref[...]
    for group in range(8):
        x = jnp.concatenate([dosage_tile(words, 4 * group + i) for i in range(4)], axis=1)
        sums = jnp.dot(left, x.astype(BF16), preferred_element_type=F32)
        squares = jnp.dot(left_tail, (x * x).astype(BF16), preferred_element_type=F32)[1:2]
        first = sums[COUNT : COUNT + 1]
        centre = rounded(first * rate)
        centred = sums - column * centre
        lower = stacked(
            [
                centred[PHENO : PHENO + 1],
                *two_parts(first),
                *two_parts(squares),
                jnp.broadcast_to(rate, first.shape),
                totals_row,
            ],
            8,
        )
        out_ref[group] = jnp.concatenate([centred[:64], lower], axis=0).astype(BF16)


def lane_group(shape):
    return lax.broadcasted_iota(jnp.int32, shape, 1) // 32


def regroup_kernel(in_ref, out_ref):
    total = jnp.zeros((ROWS, 512), F32)
    centres, parts = [], [[], [], []]
    for d in range(8):
        block = in_ref[d].astype(F32)
        total = total + block
        first = block[FIRST : FIRST + 1] + block[FIRST + 1 : FIRST + 2]
        centres.append(first * block[RATE : RATE + 1])
        for s in range(3):
            parts[s].append(block[TOTALS : TOTALS + 1, 128 * s : 128 * s + 128])
    centre8 = stacked(centres, 8)
    left = jnp.concatenate([stacked(rows, 8) for rows in parts], axis=0)
    totals = jnp.sum(left, axis=0, keepdims=True)
    lane = lax.broadcasted_iota(jnp.int32, totals.shape, 1)
    weight = jnp.sum(jnp.where(lane == COUNT, totals, 0.0), axis=1, keepdims=True)
    rate = rate_of(weight)
    first = total[FIRST : FIRST + 1] + total[FIRST + 1 : FIRST + 2]
    squares = total[SQUARE : SQUARE + 1] + total[SQUARE + 1 : SQUARE + 2]
    centre = jnp.broadcast_to(first * rate, (8, 512))
    right = jnp.concatenate([centre8] * 3 + [centre] * 3, axis=0).astype(BF16)
    left = jnp.concatenate([left, -left], axis=0).astype(BF16)
    centred = total + dot_tn(left, right)[:ROWS]
    lower = stacked(
        [
            centred[PHENO : PHENO + 1],
            *two_parts(first),
            *two_parts(squares),
            jnp.broadcast_to(rate, first.shape),
        ],
        8,
    )
    full = jnp.concatenate([centred[:64], lower], axis=0)
    rows = []
    for part in three_parts(totals):
        for k in range(3):
            rows.append(pltpu.roll(part, (96 - 24 * k) % 128, 1) if 96 - 24 * k else part)
    totals_block = stacked(rows, 24)
    group = lane_group((24, 128))
    for tile in range(4):
        blocks = [full[24 * k : 24 * k + 24, 128 * tile : 128 * tile + 128] for k in range(3)]
        for q in range(4):
            packed = totals_block
            for k in range(3):
                shift = (32 * (k - q)) % 128
                moved = pltpu.roll(blocks[k], shift, 1) if shift else blocks[k]
                packed = jnp.where(group == k, moved, packed)
            out_ref[4 * tile + q] = packed.astype(BF16)


def finish_kernel(place_ref, comp_ref, in_ref, coef_ref, extra_ref):
    total = jnp.zeros((24, 128), F32)
    group16 = lane_group((16, 128))
    lane16 = lax.broadcasted_iota(jnp.int32, (16, 128), 1)
    centres, parts = [], [[] for _ in range(9)]
    for d in range(16):
        block = in_ref[d].astype(F32)
        total = total + block
        first = block[FIRST - 48 : FIRST - 47] + block[FIRST - 47 : FIRST - 46]
        centres.append(first * block[RATE - 48 : RATE - 47])
        for i in range(9):
            parts[i].append(block[i : i + 1])
    centre16 = jnp.where(group16 == 2, rounded(stacked(centres, 16)), 0.0)
    kept = (lane16 >= 96) & (lane16 < 120)
    left = jnp.concatenate([jnp.where(kept, stacked(rows, 16), 0.0) for rows in parts], axis=0)
    moved = [pltpu.roll(centre16, 64, 1), pltpu.roll(centre16, 96, 1), centre16]
    marks = [(group16 == k).astype(F32) for k in range(3)]
    right = jnp.concatenate(
        [jnp.concatenate(moved * 3, axis=0), jnp.concatenate(marks * 3, axis=0)], axis=1
    )
    outer = dot_tn(left.astype(BF16), right.astype(BF16))[96:120]
    cross = total + outer[:, :128]
    column_totals = outer[:, 128:]
    group1 = lane_group((1, 128))
    here = group1 == 2
    weight = column_totals[COUNT - 48 : COUNT - 47]
    weight = jnp.where(here, weight, 1.0)
    first = total[FIRST - 48 : FIRST - 47] + total[FIRST - 47 : FIRST - 46]
    squares = total[SQUARE - 48 : SQUARE - 47] + total[SQUARE - 47 : SQUARE - 46]
    average = jnp.where(here, first / weight, 0.0)
    second = jnp.where(here, squares / weight, 0.0)
    spread = jnp.where(here, 1.0 / jnp.sqrt(second - average * average + EPSILON), 0.0)

    def everywhere(row):
        return row + pltpu.roll(row, 64, 1) + pltpu.roll(row, 96, 1)

    spread_all = everywhere(spread)
    unit = spread_all * (cross - everywhere(average) * column_totals)
    lane1 = lax.broadcasted_iota(jnp.int32, (1, 128), 1)
    comps = comp_ref[...]
    comp = jnp.sum(jnp.where(lane1 == place_ref[0], comps, 0), axis=1, keepdims=True)
    size = 128.0 * jnp.sum((comps == comp).astype(F32), axis=1, keepdims=True)
    inverse = 1.0 / size
    coefficients = spread_all * unit * inverse
    pheno_unit = jnp.where(here, unit[PHENO - 48 : PHENO - 47], 0.0)
    energy = jnp.sum(pheno_unit * pheno_unit * inverse, axis=1, keepdims=True)
    parts = three_parts(average)
    row = lax.broadcasted_iota(jnp.int32, (24, 128), 0)
    group = lane_group((24, 128))
    last = jnp.where(row < 16, coefficients, stacked([average] * 16 + list(parts), 24))
    packed = jnp.where(group == 2, last, jnp.where(group < 2, coefficients, 0.0)).astype(BF16)
    for d in range(16):
        coef_ref[d] = packed
    weight_all = jnp.sum(jnp.where(lane1 == 64, weight, 0.0), axis=1, keepdims=True)
    extra_ref[...] = stacked(
        [
            jnp.where(lane1 == 64 + comp, energy, 0.0),
            jnp.broadcast_to(weight_all, (1, 128)),
        ],
        8,
    )


def images_kernel(place_ref, comp_ref, words_ref, counts_ref, coef_ref, out_ref, acc_ref):
    acc_ref[...] = jnp.zeros_like(acc_ref)
    words = words_ref[...]
    group = lane_group((24, 128))
    first_tile = place_ref[1]
    for tile in range(32):
        blocks = [coef_ref[tile // 4, 4 * (tile % 4) + q].astype(F32) for q in range(4)]
        rows = []
        for k in range(3):
            row = None
            for q in range(4):
                shift = (32 * (q - k)) % 128
                moved = pltpu.roll(blocks[q], shift, 1) if shift else blocks[q]
                row = moved if row is None else jnp.where(group == q, moved, row)
            rows.append(row)
        weights = jnp.concatenate(rows, axis=0)
        x = jnp.concatenate([dosage_tile(words, tile), weights[64:72]], axis=0).astype(BF16)
        product = dot_nt(x, weights[:64].astype(BF16))
        comp = comp_ref[first_tile + tile]
        acc_ref[comp] = acc_ref[comp] + product
    root = jnp.sqrt(counts_ref[...].astype(F32))
    column = jnp.broadcast_to(root, (128, root.shape[1])).T
    for pair in range(4):
        halves = []
        for k in (2 * pair, 2 * pair + 1):
            total = acc_ref[k]
            centre = total[256:257] + total[257:258] + total[258:259]
            halves.append(total[:256] - centre)
        out_ref[:, 128 * pair : 128 * pair + 128] = (
            jnp.concatenate(halves, axis=1) * column
        ).astype(BF16)


def trace_places():
    low, high = np.zeros((24, 128), np.float32), np.zeros((24, 128), np.float32)
    r = 0
    for turned in (0, 1):
        for a in range(4):
            for b in range(a, 4):
                for table, k, l in (
                    (low, 2 * a, 2 * b + turned),
                    (high, 2 * a + 1, 2 * b + 1 - turned),
                ):
                    if turned and a == b and table is high:
                        continue
                    table[r, 8 * k + l] = 1.0
                    table[r, 8 * l + k] = 1.0
                r += 1
    return low, high


def trace_kernel(in_ref, extra_ref, low_ref, high_ref, images_ref, sums_ref):
    full = in_ref[0].astype(F32)
    for d in range(1, 4):
        full = full + in_ref[d].astype(F32)
    images_ref[...] = full.astype(BF16)
    tiles = [full[:, 128 * a : 128 * a + 128] for a in range(4)]
    turned = [pltpu.roll(t, 64, 1) for t in tiles]
    rows = []
    for others in (tiles, turned):
        for a in range(4):
            for b in range(a, 4):
                rows.append(jnp.sum(tiles[a] * others[b], axis=0, keepdims=True))
    products = stacked(rows, 24)
    lane = lax.broadcasted_iota(jnp.int32, products.shape, 1)
    low = jnp.sum(jnp.where(lane < 64, products, 0.0), axis=1, keepdims=True)
    high = jnp.sum(jnp.where(lane < 64, 0.0, products), axis=1, keepdims=True)
    sums = jnp.sum(low * low_ref[...] + high * high_ref[...], axis=0, keepdims=True)
    sums = sums + extra_ref[0:1]
    sums_ref[...] = jnp.broadcast_to(sums[None], sums_ref.shape)


def call(kernel, out, scalars=0, **kwargs):
    def run(*args):
        specs = [pl.BlockSpec(memory_space=pltpu.SMEM)] * scalars
        specs += [pl.BlockSpec(memory_space=pltpu.VMEM)] * (len(args) - scalars)
        return pl.pallas_call(kernel, out_shape=out, in_specs=specs, **kwargs)(*args)

    return run


def shape(dims, dtype):
    return jax.ShapeDtypeStruct(dims, dtype)


def on_device(geno_words, counts, probes, phenotype, tile_comp):
    y, c, x = lax.axis_index("y"), lax.axis_index("c"), lax.axis_index("x")
    z = lax.axis_index("z")
    first_tile = 32 * x
    place = jnp.stack([first_tile + 4 * (2 * y + c) + z // 4, first_tile]).astype(jnp.int32)
    counts_row = counts.reshape(1, -1)
    comp_row = tile_comp.reshape(1, -1)
    sent = call(panel_kernel, shape((8, ROWS, 512), BF16))(
        geno_words, probes, counts_row, phenotype.reshape(1, -1)
    )
    got = lax.all_to_all(sent, ("y", "c"), 0, 0, tiled=True)
    sent = call(regroup_kernel, shape((16, 24, 128), BF16))(got)
    got = lax.all_to_all(sent, "z", 0, 0, tiled=True)
    sent, extra = call(
        finish_kernel, (shape((16, 24, 128), BF16), shape((8, 128), F32)), scalars=1
    )(place, comp_row, got)
    got = lax.all_to_all(sent, "z", 0, 0, tiled=True)
    coefficients = lax.all_gather(got, ("y", "c"))
    partial = call(
        images_kernel,
        shape((256, COMPS * PROBES), BF16),
        scalars=2,
        scratch_shapes=[pltpu.VMEM((COMPS, 264, PROBES), F32)],
    )(place, tile_comp, geno_words, counts_row, coefficients)
    pieces = lax.all_to_all(partial.reshape(4, 64, COMPS * PROBES), "x", 0, 0, tiled=True)
    low, high = trace_places()
    images, sums = call(
        trace_kernel, (shape((64, COMPS * PROBES), BF16), shape((16, 1, 128), F32))
    )(pieces, extra, jnp.asarray(low), jnp.asarray(high))
    sums = jnp.sum(lax.all_to_all(sums, "z", 0, 0, tiled=True), axis=0)
    sums = jnp.broadcast_to(sums[None], (32, 1, 128))
    sums = jnp.sum(lax.all_to_all(sums, ("y", "c", "x"), 0, 0, tiled=True), axis=0)[0]
    weight_total = extra[1, 0]
    traces = sums[:64].reshape(8, 8) * (SNPS / (COMPS * PROBES)) / (weight_total * weight_total)
    return images, traces, sums[64:72] / weight_total


def solution(mesh):
    split = Mesh(mesh.devices.reshape(16, 4, 2, 4), ("z", "y", "c", "x"))
    samples = ("z", "y", "c")
    return jax.shard_map(
        on_device,
        mesh=split,
        in_specs=(P(samples, "x"), P(samples), P(samples, None), P(samples), P()),
        out_specs=(P((*samples, "x"), None), P(), P()),
        check_vma=False,
    )
```

```python
import jax
import jax.numpy as jnp
import numpy as np
from jax import lax
from jax.experimental import pallas as pl
from jax.experimental.pallas import tpu as pltpu
from jax.sharding import Mesh
from jax.sharding import PartitionSpec as P

SNPS = 16384
COMPS = 8
PROBES = 64
EPSILON = 1e-05
F32 = jnp.float32
BF16 = jnp.bfloat16

PHENO, FIRST, SQUARE, RATE, TOTALS = 64, 65, 67, 69, 70
COUNT = 65
ROWS = 72


def rounded(v):
    return v.astype(BF16).astype(F32)


def two_parts(v):
    high = rounded(v)
    return high, v - high


def three_parts(v):
    high = rounded(v)
    rest = v - high
    mid = rounded(rest)
    return high, mid, rest - mid


def stacked(rows, height):
    width = rows[0].shape[1]
    at = lax.broadcasted_iota(jnp.int32, (height, width), 0)
    out = jnp.zeros((height, width), F32)
    for i, row in enumerate(rows):
        out = jnp.where(at == i, jnp.broadcast_to(row, (height, width)), out)
    return out


def rate_of(weight):
    return rounded(1.0 / jnp.maximum(weight, 1.0))


def dot_tn(a, b):
    return lax.dot_general(a, b, (((0,), (0,)), ((), ())), preferred_element_type=F32)


def dot_nt(a, b):
    return lax.dot_general(a, b, (((1,), (1,)), ((), ())), preferred_element_type=F32)


def dosage_tile(words, tile):
    half, field = divmod(tile, 16)
    block = words[:, 128 * half : 128 * half + 128]
    return (lax.shift_right_logical(block, jnp.int32(2 * field)) & 3).astype(F32)


def panel_kernel(words_ref, probes_ref, counts_ref, pheno_ref, out_ref):
    counts = counts_ref[...].astype(F32)
    root = jnp.sqrt(counts)
    probe_rows = rounded(probes_ref[...].astype(F32) * root)
    pheno_rows = rounded(pheno_ref[...] * root)
    tail = stacked([pheno_rows, counts], 64)
    left_all = jnp.concatenate([probe_rows, tail], axis=0)
    left = left_all[:ROWS].astype(BF16)
    left_tail = left_all[64:72].astype(BF16)
    totals = dot_nt(jnp.ones((8, left_all.shape[1]), BF16), left_all.astype(BF16))[:1]
    column = jnp.sum(left_all[:ROWS], axis=1, keepdims=True)
    rate = rate_of(jnp.sum(counts, axis=1, keepdims=True))
    parts = three_parts(totals)
    totals_row = jnp.concatenate([*parts, jnp.zeros_like(totals)], axis=1)
    words = words_ref[...]
    for group in range(8):
        x = jnp.concatenate([dosage_tile(words, 4 * group + i) for i in range(4)], axis=1)
        sums = jnp.dot(left, x.astype(BF16), preferred_element_type=F32)
        squares = jnp.dot(left_tail, (x * x).astype(BF16), preferred_element_type=F32)[1:2]
        first = sums[COUNT : COUNT + 1]
        centre = rounded(first * rate)
        centred = sums - column * centre
        lower = stacked(
            [
                centred[PHENO : PHENO + 1],
                *two_parts(first),
                *two_parts(squares),
                jnp.broadcast_to(rate, first.shape),
                totals_row,
            ],
            8,
        )
        out_ref[group] = jnp.concatenate([centred[:64], lower], axis=0).astype(BF16)


def lane_group(shape):
    return lax.broadcasted_iota(jnp.int32, shape, 1) // 32


def regroup_kernel(in_ref, out_ref):
    total = jnp.zeros((ROWS, 512), F32)
    centres, parts = [], [[], [], []]
    for d in range(8):
        block = in_ref[d].astype(F32)
        total = total + block
        first = block[FIRST : FIRST + 1] + block[FIRST + 1 : FIRST + 2]
        centres.append(first * block[RATE : RATE + 1])
        for s in range(3):
            parts[s].append(block[TOTALS : TOTALS + 1, 128 * s : 128 * s + 128])
    centre8 = stacked(centres, 8)
    left = jnp.concatenate([stacked(rows, 8) for rows in parts], axis=0)
    totals = jnp.sum(left, axis=0, keepdims=True)
    lane = lax.broadcasted_iota(jnp.int32, totals.shape, 1)
    weight = jnp.sum(jnp.where(lane == COUNT, totals, 0.0), axis=1, keepdims=True)
    rate = rate_of(weight)
    first = total[FIRST : FIRST + 1] + total[FIRST + 1 : FIRST + 2]
    squares = total[SQUARE : SQUARE + 1] + total[SQUARE + 1 : SQUARE + 2]
    centre = jnp.broadcast_to(first * rate, (8, 512))
    right = jnp.concatenate([centre8] * 3 + [centre] * 3, axis=0).astype(BF16)
    left = jnp.concatenate([left, -left], axis=0).astype(BF16)
    centred = total + dot_tn(left, right)[:ROWS]
    lower = stacked(
        [
            centred[PHENO : PHENO + 1],
            *two_parts(first),
            *two_parts(squares),
            jnp.broadcast_to(rate, first.shape),
        ],
        8,
    )
    full = jnp.concatenate([centred[:64], lower], axis=0)
    rows = []
    for part in three_parts(totals):
        for k in range(3):
            rows.append(pltpu.roll(part, (96 - 24 * k) % 128, 1) if 96 - 24 * k else part)
    totals_block = stacked(rows, 24)
    group = lane_group((24, 128))
    for tile in range(4):
        blocks = [full[24 * k : 24 * k + 24, 128 * tile : 128 * tile + 128] for k in range(3)]
        for q in range(4):
            packed = totals_block
            for k in range(3):
                shift = (32 * (k - q)) % 128
                moved = pltpu.roll(blocks[k], shift, 1) if shift else blocks[k]
                packed = jnp.where(group == k, moved, packed)
            out_ref[4 * tile + q] = packed.astype(BF16)


def finish_kernel(comp_ref, in_ref, coef_ref, extra_ref):
    total = jnp.zeros((24, 128), F32)
    group16 = lane_group((16, 128))
    lane16 = lax.broadcasted_iota(jnp.int32, (16, 128), 1)
    centres, parts = [], [[] for _ in range(9)]
    for d in range(16):
        block = in_ref[d].astype(F32)
        total = total + block
        first = block[FIRST - 48 : FIRST - 47] + block[FIRST - 47 : FIRST - 46]
        centres.append(first * block[RATE - 48 : RATE - 47])
        for i in range(9):
            parts[i].append(block[i : i + 1])
    centre16 = jnp.where(group16 == 2, rounded(stacked(centres, 16)), 0.0)
    kept = (lane16 >= 96) & (lane16 < 120)
    left = jnp.concatenate([jnp.where(kept, stacked(rows, 16), 0.0) for rows in parts], axis=0)
    moved = [pltpu.roll(centre16, 64, 1), pltpu.roll(centre16, 96, 1), centre16]
    marks = [(group16 == k).astype(F32) for k in range(3)]
    right = jnp.concatenate(
        [jnp.concatenate(moved * 3, axis=0), jnp.concatenate(marks * 3, axis=0)], axis=1
    )
    outer = dot_tn(left.astype(BF16), right.astype(BF16))[96:120]
    cross = total + outer[:, :128]
    column_totals = outer[:, 128:]
    group1 = lane_group((1, 128))
    here = group1 == 2
    weight = column_totals[COUNT - 48 : COUNT - 47]
    weight = jnp.where(here, weight, 1.0)
    first = total[FIRST - 48 : FIRST - 47] + total[FIRST - 47 : FIRST - 46]
    squares = total[SQUARE - 48 : SQUARE - 47] + total[SQUARE - 47 : SQUARE - 46]
    average = jnp.where(here, first / weight, 0.0)
    second = jnp.where(here, squares / weight, 0.0)
    spread = jnp.where(here, 1.0 / jnp.sqrt(second - average * average + EPSILON), 0.0)

    def everywhere(row):
        return row + pltpu.roll(row, 64, 1) + pltpu.roll(row, 96, 1)

    spread_all = everywhere(spread)
    unit = spread_all * (cross - everywhere(average) * column_totals)
    lane1 = lax.broadcasted_iota(jnp.int32, (1, 128), 1)
    z, y, c, x = (lax.axis_index(name) for name in "zycx")
    tile = 32 * x + 8 * y + 4 * c + lax.shift_right_logical(z, 2)
    comps = comp_ref[...]
    comp = jnp.sum(jnp.where(lane1 == tile, comps, 0), axis=1, keepdims=True)
    size = 128.0 * jnp.sum((comps == comp).astype(F32), axis=1, keepdims=True)
    inverse = 1.0 / size
    coefficients = spread_all * unit * inverse
    pheno_unit = jnp.where(here, unit[PHENO - 48 : PHENO - 47], 0.0)
    energy = jnp.sum(pheno_unit * pheno_unit * inverse, axis=1, keepdims=True)
    parts = three_parts(average)
    row = lax.broadcasted_iota(jnp.int32, (24, 128), 0)
    group = lane_group((24, 128))
    last = jnp.where(row < 16, coefficients, stacked([average] * 16 + list(parts), 24))
    packed = jnp.where(group == 2, last, jnp.where(group < 2, coefficients, 0.0)).astype(BF16)
    for d in range(16):
        coef_ref[d] = packed
    weight_all = jnp.sum(jnp.where(lane1 == 64, weight, 0.0), axis=1, keepdims=True)
    extra_ref[...] = stacked(
        [
            jnp.where(lane1 == 64 + comp, energy, 0.0),
            jnp.broadcast_to(weight_all, (1, 128)),
        ],
        8,
    )


def unpack_kernel(in_ref, out_ref):
    group = lane_group((24, 128))
    for tile in range(4):
        blocks = [in_ref[4 * tile + q].astype(F32) for q in range(4)]
        rows = []
        for k in range(3):
            row = None
            for q in range(4):
                shift = (32 * (q - k)) % 128
                moved = pltpu.roll(blocks[q], shift, 1) if shift else blocks[q]
                row = moved if row is None else jnp.where(group == q, moved, row)
            rows.append(row)
        whole = jnp.concatenate(rows, axis=0).astype(BF16)
        for d in range(4):
            out_ref[d, :, 128 * tile : 128 * tile + 128] = whole


def images_kernel(comp_ref, words_ref, counts_ref, coef_ref, out_ref, acc_ref):
    acc_ref[...] = jnp.zeros_like(acc_ref)
    words = words_ref[...]
    first_tile = 32 * lax.axis_index("x")
    for tile in range(32):
        y, c = divmod(tile // 4, 2)
        at = 128 * (tile % 4)
        weights = coef_ref[c, y, :, at : at + 128].astype(F32)
        x = jnp.concatenate([dosage_tile(words, tile), weights[64:72]], axis=0).astype(BF16)
        product = dot_nt(x, weights[:64].astype(BF16))
        comp = comp_ref[first_tile + tile]
        acc_ref[comp] = acc_ref[comp] + product
    root = jnp.sqrt(counts_ref[...].astype(F32))
    column = jnp.broadcast_to(root, (128, root.shape[1])).T
    for pair in range(4):
        halves = []
        for k in (2 * pair, 2 * pair + 1):
            total = acc_ref[k]
            centre = total[256:257] + total[257:258] + total[258:259]
            halves.append(total[:256] - centre)
        out_ref[:, 128 * pair : 128 * pair + 128] = (
            jnp.concatenate(halves, axis=1) * column
        ).astype(BF16)


def trace_places():
    low, high = np.zeros((24, 128), np.float32), np.zeros((24, 128), np.float32)
    r = 0
    for turned in (0, 1):
        for a in range(4):
            for b in range(a, 4):
                for table, k, l in (
                    (low, 2 * a, 2 * b + turned),
                    (high, 2 * a + 1, 2 * b + 1 - turned),
                ):
                    if turned and a == b and table is high:
                        continue
                    table[r, 8 * k + l] = 1.0
                    table[r, 8 * l + k] = 1.0
                r += 1
    return low, high


def trace_kernel(in_ref, extra_ref, low_ref, high_ref, images_ref, sums_ref):
    full = in_ref[0].astype(F32)
    for d in range(1, 4):
        full = full + in_ref[d].astype(F32)
    images_ref[...] = full.astype(BF16)
    tiles = [full[:, 128 * a : 128 * a + 128] for a in range(4)]
    turned = [pltpu.roll(t, 64, 1) for t in tiles]
    rows = []
    for others in (tiles, turned):
        for a in range(4):
            for b in range(a, 4):
                rows.append(jnp.sum(tiles[a] * others[b], axis=0, keepdims=True))
    products = stacked(rows, 24)
    lane = lax.broadcasted_iota(jnp.int32, products.shape, 1)
    low = jnp.sum(jnp.where(lane < 64, products, 0.0), axis=1, keepdims=True)
    high = jnp.sum(jnp.where(lane < 64, 0.0, products), axis=1, keepdims=True)
    sums = jnp.sum(low * low_ref[...] + high * high_ref[...], axis=0, keepdims=True)
    sums = sums + extra_ref[0:1]
    sums_ref[...] = jnp.broadcast_to(sums[None], sums_ref.shape)


def middle_kernel(in_ref, out_ref):
    out_ref[...] = jnp.broadcast_to(jnp.sum(in_ref[...], axis=0, keepdims=True), out_ref.shape)


def last_kernel(in_ref, extra_ref, traces_ref, yky_ref):
    sums = jnp.sum(in_ref[...], axis=0)
    weight = extra_ref[1:2]
    scaled = sums * (SNPS / (COMPS * PROBES)) / (weight * weight)
    rows = [scaled] + [pltpu.roll(scaled, 128 - 8 * k, 1) for k in range(1, 8)]
    traces_ref[...] = stacked(rows, 8)[:, :8]
    yky_ref[...] = pltpu.roll(sums / weight, 64, 1)[:, :8]


def call(kernel, out, scalars=0, **kwargs):
    def run(*args):
        specs = [pl.BlockSpec(memory_space=pltpu.SMEM)] * scalars
        specs += [pl.BlockSpec(memory_space=pltpu.VMEM)] * (len(args) - scalars)
        return pl.pallas_call(kernel, out_shape=out, in_specs=specs, **kwargs)(*args)

    return run


def near(array):
    return pltpu.with_memory_space_constraint(array, pltpu.VMEM)


def shape(dims, dtype):
    return jax.ShapeDtypeStruct(dims, dtype)


def on_device(geno_words, counts, probes, phenotype, tile_comp):
    counts_row = counts.reshape(1, -1)
    comp_row = tile_comp.reshape(1, -1)
    sent = call(panel_kernel, pltpu.VMEM((8, ROWS, 512), BF16))(
        geno_words, probes.T, counts_row, phenotype.reshape(1, -1)
    )
    got = lax.all_to_all(sent, ("y", "c"), 0, 0, tiled=True)
    sent = call(regroup_kernel, pltpu.VMEM((16, 24, 128), BF16))(near(got))
    got = lax.all_to_all(sent, "z", 0, 0, tiled=True)
    sent, extra = call(
        finish_kernel, (pltpu.VMEM((16, 24, 128), BF16), pltpu.VMEM((8, 128), F32))
    )(comp_row, near(got))
    got = lax.all_to_all(sent, "z", 0, 0, tiled=True)
    sent = call(unpack_kernel, pltpu.VMEM((4, ROWS, 512), BF16))(near(got))
    got = lax.all_to_all(sent, "y", 0, 0, tiled=True)
    coefficients = lax.all_gather(got, "c")
    partial = call(
        images_kernel,
        pltpu.VMEM((256, COMPS * PROBES), BF16),
        scalars=1,
        scratch_shapes=[pltpu.VMEM((COMPS, 264, PROBES), F32)],
    )(tile_comp, geno_words, counts_row, near(coefficients))
    pieces = lax.all_to_all(partial.reshape(4, 64, COMPS * PROBES), "x", 0, 0, tiled=True)
    low, high = trace_places()
    images, sums = call(
        trace_kernel, (shape((64, COMPS * PROBES), BF16), pltpu.VMEM((16, 1, 128), F32))
    )(near(pieces), near(extra), jnp.asarray(low), jnp.asarray(high))
    got = lax.all_to_all(sums, "z", 0, 0, tiled=True)
    sums = call(middle_kernel, pltpu.VMEM((32, 1, 128), F32))(near(got))
    got = lax.all_to_all(sums, ("y", "c", "x"), 0, 0, tiled=True)
    traces, yky = call(last_kernel, (shape((8, 8), F32), shape((1, 8), F32)))(
        near(got), near(extra)
    )
    return images, traces, yky.reshape(8)


def solution(mesh):
    split = Mesh(mesh.devices.reshape(16, 4, 2, 4), ("z", "y", "c", "x"))
    samples = ("z", "y", "c")
    return jax.shard_map(
        on_device,
        mesh=split,
        in_specs=(P(samples, "x"), P(samples), P(samples, None), P(samples), P()),
        out_specs=(P((*samples, "x"), None), P(), P()),
        check_vma=False,
    )
```

```python
import jax
import jax.numpy as jnp
import numpy as np
from jax import lax
from jax.experimental import pallas as pl
from jax.experimental.pallas import tpu as pltpu
from jax.sharding import Mesh
from jax.sharding import PartitionSpec as P

SNPS = 16384
COMPS = 8
PROBES = 64
EPSILON = 1e-05
F32 = jnp.float32
BF16 = jnp.bfloat16

PHENO, FIRST, SQUARE, RATE, TOTALS = 64, 65, 67, 69, 70
COUNT = 65
ROWS = 72


def rounded(v):
    return v.astype(BF16).astype(F32)


def two_parts(v):
    high = rounded(v)
    return high, v - high


def three_parts(v):
    high = rounded(v)
    rest = v - high
    mid = rounded(rest)
    return high, mid, rest - mid


def stacked(rows, height):
    width = rows[0].shape[1]
    at = lax.broadcasted_iota(jnp.int32, (height, width), 0)
    out = jnp.zeros((height, width), F32)
    for i, row in enumerate(rows):
        out = jnp.where(at == i, jnp.broadcast_to(row, (height, width)), out)
    return out


def rate_of(weight):
    return rounded(1.0 / jnp.maximum(weight, 1.0))


def dot_tn(a, b):
    return lax.dot_general(a, b, (((0,), (0,)), ((), ())), preferred_element_type=F32)


def dot_nt(a, b):
    return lax.dot_general(a, b, (((1,), (1,)), ((), ())), preferred_element_type=F32)


def dosage_tile(words, tile):
    half, field = divmod(tile, 16)
    block = words[:, 128 * half : 128 * half + 128]
    return (lax.shift_right_logical(block, jnp.int32(2 * field)) & 3).astype(F32)


def panel_kernel(words_ref, probes_ref, counts_ref, pheno_ref, out_ref):
    counts = counts_ref[...].astype(F32)
    root = jnp.sqrt(counts)
    probe_rows = rounded(probes_ref[...].astype(F32) * root)
    pheno_rows = rounded(pheno_ref[...] * root)
    tail = stacked([pheno_rows, counts], 64)
    left_all = jnp.concatenate([probe_rows, tail], axis=0)
    left = left_all[:ROWS].astype(BF16)
    left_tail = left_all[64:72].astype(BF16)
    totals = dot_nt(jnp.ones((8, left_all.shape[1]), BF16), left_all.astype(BF16))[:1]
    column = jnp.sum(left_all[:ROWS], axis=1, keepdims=True)
    rate = rate_of(jnp.sum(counts, axis=1, keepdims=True))
    parts = three_parts(totals)
    totals_row = jnp.concatenate([*parts, jnp.zeros_like(totals)], axis=1)
    words = words_ref[...]
    for group in range(8):
        x = jnp.concatenate([dosage_tile(words, 4 * group + i) for i in range(4)], axis=1)
        sums = jnp.dot(left, x.astype(BF16), preferred_element_type=F32)
        squares = jnp.dot(left_tail, (x * x).astype(BF16), preferred_element_type=F32)[1:2]
        first = sums[COUNT : COUNT + 1]
        centre = rounded(first * rate)
        centred = sums - column * centre
        lower = stacked(
            [
                centred[PHENO : PHENO + 1],
                *two_parts(first),
                *two_parts(squares),
                jnp.broadcast_to(rate, first.shape),
                totals_row,
            ],
            8,
        )
        out_ref[group] = jnp.concatenate([centred[:64], lower], axis=0).astype(BF16)


def lane_group(shape):
    return lax.broadcasted_iota(jnp.int32, shape, 1) // 32


def regroup_kernel(in_ref, out_ref):
    total = jnp.zeros((ROWS, 512), F32)
    centres, parts = [], [[], [], []]
    for d in range(8):
        block = in_ref[d].astype(F32)
        total = total + block
        first = block[FIRST : FIRST + 1] + block[FIRST + 1 : FIRST + 2]
        centres.append(first * block[RATE : RATE + 1])
        for s in range(3):
            parts[s].append(block[TOTALS : TOTALS + 1, 128 * s : 128 * s + 128])
    centre8 = stacked(centres, 8)
    left = jnp.concatenate([stacked(rows, 8) for rows in parts], axis=0)
    totals = jnp.sum(left, axis=0, keepdims=True)
    lane = lax.broadcasted_iota(jnp.int32, totals.shape, 1)
    weight = jnp.sum(jnp.where(lane == COUNT, totals, 0.0), axis=1, keepdims=True)
    rate = rate_of(weight)
    first = total[FIRST : FIRST + 1] + total[FIRST + 1 : FIRST + 2]
    squares = total[SQUARE : SQUARE + 1] + total[SQUARE + 1 : SQUARE + 2]
    centre = jnp.broadcast_to(first * rate, (8, 512))
    right = jnp.concatenate([centre8] * 3 + [centre] * 3, axis=0).astype(BF16)
    left = jnp.concatenate([left, -left], axis=0).astype(BF16)
    centred = total + dot_tn(left, right)[:ROWS]
    lower = stacked(
        [
            centred[PHENO : PHENO + 1],
            *two_parts(first),
            *two_parts(squares),
            jnp.broadcast_to(rate, first.shape),
        ],
        8,
    )
    full = jnp.concatenate([centred[:64], lower], axis=0)
    rows = []
    for part in three_parts(totals):
        for k in range(3):
            rows.append(pltpu.roll(part, (96 - 24 * k) % 128, 1) if 96 - 24 * k else part)
    totals_block = stacked(rows, 24)
    group = lane_group((24, 128))
    for tile in range(4):
        blocks = [full[24 * k : 24 * k + 24, 128 * tile : 128 * tile + 128] for k in range(3)]
        for q in range(4):
            packed = totals_block
            for k in range(3):
                shift = (32 * (k - q)) % 128
                moved = pltpu.roll(blocks[k], shift, 1) if shift else blocks[k]
                packed = jnp.where(group == k, moved, packed)
            out_ref[4 * tile + q] = packed.astype(BF16)


def finish_kernel(comp_ref, in_ref, coef_ref, extra_ref):
    total = jnp.zeros((24, 128), F32)
    group16 = lane_group((16, 128))
    lane16 = lax.broadcasted_iota(jnp.int32, (16, 128), 1)
    centres, parts = [], [[] for _ in range(9)]
    for d in range(16):
        block = in_ref[d].astype(F32)
        total = total + block
        first = block[FIRST - 48 : FIRST - 47] + block[FIRST - 47 : FIRST - 46]
        centres.append(first * block[RATE - 48 : RATE - 47])
        for i in range(9):
            parts[i].append(block[i : i + 1])
    centre16 = jnp.where(group16 == 2, rounded(stacked(centres, 16)), 0.0)
    kept = (lane16 >= 96) & (lane16 < 120)
    left = jnp.concatenate([jnp.where(kept, stacked(rows, 16), 0.0) for rows in parts], axis=0)
    moved = [pltpu.roll(centre16, 64, 1), pltpu.roll(centre16, 96, 1), centre16]
    marks = [(group16 == k).astype(F32) for k in range(3)]
    right = jnp.concatenate(
        [jnp.concatenate(moved * 3, axis=0), jnp.concatenate(marks * 3, axis=0)], axis=1
    )
    outer = dot_tn(left.astype(BF16), right.astype(BF16))[96:120]
    cross = total + outer[:, :128]
    column_totals = outer[:, 128:]
    group1 = lane_group((1, 128))
    here = group1 == 2
    weight = column_totals[COUNT - 48 : COUNT - 47]
    weight = jnp.where(here, weight, 1.0)
    first = total[FIRST - 48 : FIRST - 47] + total[FIRST - 47 : FIRST - 46]
    squares = total[SQUARE - 48 : SQUARE - 47] + total[SQUARE - 47 : SQUARE - 46]
    average = jnp.where(here, first / weight, 0.0)
    second = jnp.where(here, squares / weight, 0.0)
    spread = jnp.where(here, 1.0 / jnp.sqrt(second - average * average + EPSILON), 0.0)

    def everywhere(row):
        return row + pltpu.roll(row, 64, 1) + pltpu.roll(row, 96, 1)

    spread_all = everywhere(spread)
    unit = spread_all * (cross - everywhere(average) * column_totals)
    lane1 = lax.broadcasted_iota(jnp.int32, (1, 128), 1)
    z, y, c, x = (lax.axis_index(name) for name in "zycx")
    tile = 32 * x + 8 * y + 4 * c + lax.shift_right_logical(z, 2)
    comps = comp_ref[...]
    comp = jnp.sum(jnp.where(lane1 == tile, comps, 0), axis=1, keepdims=True)
    size = 128.0 * jnp.sum((comps == comp).astype(F32), axis=1, keepdims=True)
    inverse = 1.0 / size
    coefficients = spread_all * unit * inverse
    pheno_unit = jnp.where(here, unit[PHENO - 48 : PHENO - 47], 0.0)
    energy = jnp.sum(pheno_unit * pheno_unit * inverse, axis=1, keepdims=True)
    parts = three_parts(average)
    row = lax.broadcasted_iota(jnp.int32, (24, 128), 0)
    group = lane_group((24, 128))
    last = jnp.where(row < 16, coefficients, stacked([average] * 16 + list(parts), 24))
    packed = jnp.where(group == 2, last, jnp.where(group < 2, coefficients, 0.0)).astype(BF16)
    for d in range(16):
        coef_ref[d] = packed
    weight_all = jnp.sum(jnp.where(lane1 == 64, weight, 0.0), axis=1, keepdims=True)
    extra_ref[...] = stacked(
        [
            jnp.where(lane1 == 64 + comp, energy, 0.0),
            jnp.broadcast_to(weight_all, (1, 128)),
        ],
        8,
    )


def unpack_kernel(in_ref, out_ref):
    group = lane_group((24, 128))
    for tile in range(4):
        blocks = [in_ref[4 * tile + q].astype(F32) for q in range(4)]
        rows = []
        for k in range(3):
            row = None
            for q in range(4):
                shift = (32 * (q - k)) % 128
                moved = pltpu.roll(blocks[q], shift, 1) if shift else blocks[q]
                row = moved if row is None else jnp.where(group == q, moved, row)
            rows.append(row)
        whole = jnp.concatenate(rows, axis=0).astype(BF16)
        for d in range(4):
            out_ref[d, :, 128 * tile : 128 * tile + 128] = whole


def images_kernel(comp_ref, words_ref, counts_ref, coef_ref, out_ref, acc_ref):
    acc_ref[...] = jnp.zeros_like(acc_ref)
    words = words_ref[...]
    first_tile = 32 * lax.axis_index("x")
    lane = lax.broadcasted_iota(jnp.int32, (264, 128), 1)
    blank = jnp.zeros((PROBES, 128), BF16)
    for tile in range(0, 32, 2):
        y, c = divmod(tile // 4, 2)
        at = 128 * (tile % 4)
        weights = coef_ref[c, y, :PROBES, at : at + 256]
        averages = coef_ref[c, y, PROBES:, at : at + 256].astype(F32)
        x = jnp.concatenate([dosage_tile(words, tile), dosage_tile(words, tile + 1)], axis=1)
        x = jnp.concatenate([x, averages], axis=0).astype(BF16)
        left = jnp.concatenate([weights[:, :128], blank], axis=1)
        right = jnp.concatenate([blank, weights[:, 128:]], axis=1)
        product = dot_nt(x, jnp.concatenate([left, right], axis=0))
        comp = comp_ref[first_tile + tile]
        acc_ref[comp] = acc_ref[comp] + jnp.where(lane < PROBES, product, 0.0)
        comp = comp_ref[first_tile + tile + 1]
        acc_ref[comp] = acc_ref[comp] + jnp.where(lane < PROBES, 0.0, product)
    root = jnp.sqrt(counts_ref[...].astype(F32))
    column = jnp.broadcast_to(root, (128, root.shape[1])).T
    for pair in range(4):
        halves = []
        for k in (2 * pair, 2 * pair + 1):
            total = acc_ref[k]
            total = total + pltpu.roll(total, PROBES, 1)
            centre = total[256:257] + total[257:258] + total[258:259]
            halves.append(total[:256] - centre)
        out_ref[:, 128 * pair : 128 * pair + 128] = (
            jnp.where(lane[:256] < PROBES, *halves) * column
        ).astype(BF16)


def trace_places():
    low, high = np.zeros((24, 128), np.float32), np.zeros((24, 128), np.float32)
    r = 0
    for turned in (0, 1):
        for a in range(4):
            for b in range(a, 4):
                for table, k, l in (
                    (low, 2 * a, 2 * b + turned),
                    (high, 2 * a + 1, 2 * b + 1 - turned),
                ):
                    if turned and a == b and table is high:
                        continue
                    table[r, 8 * k + l] = 1.0
                    table[r, 8 * l + k] = 1.0
                r += 1
    return low, high


def trace_kernel(in_ref, extra_ref, low_ref, high_ref, images_ref, sums_ref):
    full = in_ref[0].astype(F32)
    for d in range(1, 4):
        full = full + in_ref[d].astype(F32)
    images_ref[...] = full.astype(BF16)
    tiles = [full[:, 128 * a : 128 * a + 128] for a in range(4)]
    turned = [pltpu.roll(t, 64, 1) for t in tiles]
    rows = []
    for others in (tiles, turned):
        for a in range(4):
            for b in range(a, 4):
                rows.append(jnp.sum(tiles[a] * others[b], axis=0, keepdims=True))
    products = stacked(rows, 24)
    lane = lax.broadcasted_iota(jnp.int32, products.shape, 1)
    low = jnp.sum(jnp.where(lane < 64, products, 0.0), axis=1, keepdims=True)
    high = jnp.sum(jnp.where(lane < 64, 0.0, products), axis=1, keepdims=True)
    sums = jnp.sum(low * low_ref[...] + high * high_ref[...], axis=0, keepdims=True)
    sums = sums + extra_ref[0:1]
    sums_ref[...] = jnp.broadcast_to(sums[None], sums_ref.shape)


def middle_kernel(in_ref, out_ref):
    out_ref[...] = jnp.broadcast_to(jnp.sum(in_ref[...], axis=0, keepdims=True), out_ref.shape)


def last_kernel(in_ref, extra_ref, held_ref, images_ref, traces_ref, yky_ref):
    images_ref[...] = held_ref[...]
    sums = jnp.sum(in_ref[...], axis=0)
    weight = extra_ref[1:2]
    scaled = sums * (SNPS / (COMPS * PROBES)) / (weight * weight)
    rows = [scaled] + [pltpu.roll(scaled, 128 - 8 * k, 1) for k in range(1, 8)]
    traces_ref[...] = stacked(rows, 8)[:, :8]
    yky_ref[...] = pltpu.roll(sums / weight, 64, 1)[:, :8]


def call(kernel, out, scalars=0, **kwargs):
    def run(*args):
        specs = [pl.BlockSpec(memory_space=pltpu.SMEM)] * scalars
        specs += [pl.BlockSpec(memory_space=pltpu.VMEM)] * (len(args) - scalars)
        return pl.pallas_call(kernel, out_shape=out, in_specs=specs, **kwargs)(*args)

    return run


def near(array):
    return pltpu.with_memory_space_constraint(array, pltpu.VMEM)


def shape(dims, dtype):
    return jax.ShapeDtypeStruct(dims, dtype)


def on_device(geno_words, counts, probes, phenotype, tile_comp):
    counts_row = counts.reshape(1, -1)
    comp_row = tile_comp.reshape(1, -1)
    sent = call(panel_kernel, pltpu.VMEM((8, ROWS, 512), BF16))(
        geno_words, probes.T, counts_row, phenotype.reshape(1, -1)
    )
    got = lax.all_to_all(sent, ("y", "c"), 0, 0, tiled=True)
    sent = call(regroup_kernel, pltpu.VMEM((16, 24, 128), BF16))(near(got))
    got = lax.all_to_all(sent, "z", 0, 0, tiled=True)
    sent, extra = call(
        finish_kernel, (pltpu.VMEM((16, 24, 128), BF16), pltpu.VMEM((8, 128), F32))
    )(near(comp_row), near(got))
    got = lax.all_to_all(sent, "z", 0, 0, tiled=True)
    sent = call(unpack_kernel, pltpu.VMEM((4, ROWS, 512), BF16))(near(got))
    got = lax.all_to_all(sent, "y", 0, 0, tiled=True)
    coefficients = lax.all_gather(got, "c")
    partial = call(
        images_kernel,
        pltpu.VMEM((256, COMPS * PROBES), BF16),
        scalars=1,
        scratch_shapes=[pltpu.VMEM((COMPS, 264, 128), F32)],
    )(tile_comp, near(geno_words), near(counts_row), near(coefficients))
    pieces = lax.all_to_all(partial.reshape(4, 64, COMPS * PROBES), "x", 0, 0, tiled=True)
    low, high = trace_places()
    images, sums = call(
        trace_kernel, (pltpu.VMEM((64, COMPS * PROBES), BF16), pltpu.VMEM((16, 1, 128), F32))
    )(near(pieces), near(extra), near(jnp.asarray(low)), near(jnp.asarray(high)))
    got = lax.all_to_all(sums, "z", 0, 0, tiled=True)
    sums = call(middle_kernel, pltpu.VMEM((32, 1, 128), F32))(near(got))
    got = lax.all_to_all(sums, ("y", "c", "x"), 0, 0, tiled=True)
    images, traces, yky = call(
        last_kernel,
        (shape((64, COMPS * PROBES), BF16), shape((8, 8), F32), shape((1, 8), F32)),
    )(near(got), near(extra), near(images))
    return images, traces, yky.reshape(8)


def solution(mesh):
    split = Mesh(mesh.devices.reshape(16, 4, 2, 4), ("z", "y", "c", "x"))
    samples = ("z", "y", "c")
    return jax.shard_map(
        on_device,
        mesh=split,
        in_specs=(P(samples, "x"), P(samples), P(samples, None), P(samples), P()),
        out_specs=(P((*samples, "x"), None), P(), P()),
        check_vma=False,
    )
```

```python
import jax
import jax.numpy as jnp
import numpy as np
from jax import lax
from jax.experimental import pallas as pl
from jax.experimental.pallas import tpu as pltpu
from jax.sharding import Mesh
from jax.sharding import PartitionSpec as P

SNPS = 16384
COMPS = 8
PROBES = 64
EPSILON = 1e-05
F32 = jnp.float32
BF16 = jnp.bfloat16

PHENO, FIRST, SQUARE, RATE, TOTALS = 64, 65, 67, 69, 70
COUNT = 65
ROWS = 72


def rounded(v):
    return v.astype(BF16).astype(F32)


def two_parts(v):
    high = rounded(v)
    return high, v - high


def three_parts(v):
    high = rounded(v)
    rest = v - high
    mid = rounded(rest)
    return high, mid, rest - mid


def stacked(rows, height):
    width = rows[0].shape[1]
    at = lax.broadcasted_iota(jnp.int32, (height, width), 0)
    out = jnp.zeros((height, width), F32)
    for i, row in enumerate(rows):
        out = jnp.where(at == i, jnp.broadcast_to(row, (height, width)), out)
    return out


def rate_of(weight):
    return rounded(1.0 / jnp.maximum(weight, 1.0))


def dot_tn(a, b):
    return lax.dot_general(a, b, (((0,), (0,)), ((), ())), preferred_element_type=F32)


def dot_nt(a, b):
    return lax.dot_general(a, b, (((1,), (1,)), ((), ())), preferred_element_type=F32)


def dosage_tile(words, tile):
    half, field = divmod(tile, 16)
    block = words[:, 128 * half : 128 * half + 128]
    return (lax.shift_right_logical(block, jnp.int32(2 * field)) & 3).astype(F32)


def panel_kernel(
    comp_ref, words_ref, probes_ref, counts_ref, pheno_ref, comps_ref, out_ref, root_ref, held_ref, own_ref
):
    held_ref[...] = comps_ref[...]
    first_tile = 32 * lax.axis_index("x")
    for tile in range(32):
        own_ref[tile] = comp_ref[first_tile + tile]
    counts = counts_ref[...].astype(F32)
    root = jnp.sqrt(counts)
    root_ref[...] = root
    probe_rows = rounded(probes_ref[...].astype(F32) * root)
    pheno_rows = rounded(pheno_ref[...] * root)
    tail = stacked([pheno_rows, counts], 64)
    left_all = jnp.concatenate([probe_rows, tail], axis=0)
    left = left_all[:ROWS].astype(BF16)
    left_tail = left_all[64:72].astype(BF16)
    totals = dot_nt(jnp.ones((8, left_all.shape[1]), BF16), left_all.astype(BF16))[:1]
    column = jnp.sum(left_all[:ROWS], axis=1, keepdims=True)
    rate = rate_of(jnp.sum(counts, axis=1, keepdims=True))
    parts = three_parts(totals)
    totals_row = jnp.concatenate([*parts, jnp.zeros_like(totals)], axis=1)
    words = words_ref[...]
    for group in range(8):
        x = jnp.concatenate([dosage_tile(words, 4 * group + i) for i in range(4)], axis=1)
        x = x.astype(BF16)
        sums = jnp.dot(left, x, preferred_element_type=F32)
        squares = jnp.dot(left_tail, x * x, preferred_element_type=F32)[1:2]
        first = sums[COUNT : COUNT + 1]
        centre = rounded(first * rate)
        centred = sums - column * centre
        lower = stacked(
            [
                centred[PHENO : PHENO + 1],
                *two_parts(first),
                *two_parts(squares),
                jnp.broadcast_to(rate, first.shape),
                totals_row,
            ],
            8,
        )
        out_ref[group] = jnp.concatenate([centred[:64], lower], axis=0).astype(BF16)


def lane_group(shape):
    return lax.broadcasted_iota(jnp.int32, shape, 1) // 32


def regroup_kernel(in_ref, out_ref):
    total = jnp.zeros((ROWS, 512), F32)
    centres, parts = [], [[], [], []]
    for d in range(8):
        block = in_ref[d].astype(F32)
        total = total + block
        first = block[FIRST : FIRST + 1] + block[FIRST + 1 : FIRST + 2]
        centres.append(first * block[RATE : RATE + 1])
        for s in range(3):
            parts[s].append(block[TOTALS : TOTALS + 1, 128 * s : 128 * s + 128])
    centre8 = stacked(centres, 8)
    left = jnp.concatenate([stacked(rows, 8) for rows in parts], axis=0)
    totals = jnp.sum(left, axis=0, keepdims=True)
    lane = lax.broadcasted_iota(jnp.int32, totals.shape, 1)
    weight = jnp.sum(jnp.where(lane == COUNT, totals, 0.0), axis=1, keepdims=True)
    rate = rate_of(weight)
    first = total[FIRST : FIRST + 1] + total[FIRST + 1 : FIRST + 2]
    squares = total[SQUARE : SQUARE + 1] + total[SQUARE + 1 : SQUARE + 2]
    centre = jnp.broadcast_to(first * rate, (8, 512))
    right = jnp.concatenate([centre8] * 3 + [centre] * 3, axis=0).astype(BF16)
    left = jnp.concatenate([left, -left], axis=0).astype(BF16)
    centred = total + dot_tn(left, right)[:ROWS]
    lower = stacked(
        [
            centred[PHENO : PHENO + 1],
            *two_parts(first),
            *two_parts(squares),
            jnp.broadcast_to(rate, first.shape),
        ],
        8,
    )
    full = jnp.concatenate([centred[:64], lower], axis=0)
    rows = []
    for part in three_parts(totals):
        for k in range(3):
            rows.append(pltpu.roll(part, (96 - 24 * k) % 128, 1) if 96 - 24 * k else part)
    totals_block = stacked(rows, 24)
    group = lane_group((24, 128))
    for tile in range(4):
        blocks = [full[24 * k : 24 * k + 24, 128 * tile : 128 * tile + 128] for k in range(3)]
        for q in range(4):
            packed = totals_block
            for k in range(3):
                shift = (32 * (k - q)) % 128
                moved = pltpu.roll(blocks[k], shift, 1) if shift else blocks[k]
                packed = jnp.where(group == k, moved, packed)
            out_ref[4 * tile + q] = packed.astype(BF16)


def finish_kernel(comp_ref, in_ref, coef_ref, extra_ref):
    total = jnp.zeros((24, 128), F32)
    group16 = lane_group((16, 128))
    lane16 = lax.broadcasted_iota(jnp.int32, (16, 128), 1)
    centres, parts = [], [[] for _ in range(9)]
    for d in range(16):
        block = in_ref[d].astype(F32)
        total = total + block
        first = block[FIRST - 48 : FIRST - 47] + block[FIRST - 47 : FIRST - 46]
        centres.append(first * block[RATE - 48 : RATE - 47])
        for i in range(9):
            parts[i].append(block[i : i + 1])
    centre16 = jnp.where(group16 == 2, rounded(stacked(centres, 16)), 0.0)
    kept = (lane16 >= 96) & (lane16 < 120)
    left = jnp.concatenate([jnp.where(kept, stacked(rows, 16), 0.0) for rows in parts], axis=0)
    moved = [pltpu.roll(centre16, 64, 1), pltpu.roll(centre16, 96, 1), centre16]
    marks = [(group16 == k).astype(F32) for k in range(3)]
    right = jnp.concatenate(
        [jnp.concatenate(moved * 3, axis=0), jnp.concatenate(marks * 3, axis=0)], axis=1
    )
    outer = dot_tn(left.astype(BF16), right.astype(BF16))[96:120]
    cross = total + outer[:, :128]
    column_totals = outer[:, 128:]
    group1 = lane_group((1, 128))
    here = group1 == 2
    weight = column_totals[COUNT - 48 : COUNT - 47]
    weight = jnp.where(here, weight, 1.0)
    first = total[FIRST - 48 : FIRST - 47] + total[FIRST - 47 : FIRST - 46]
    squares = total[SQUARE - 48 : SQUARE - 47] + total[SQUARE - 47 : SQUARE - 46]
    average = jnp.where(here, first / weight, 0.0)
    second = jnp.where(here, squares / weight, 0.0)
    spread = jnp.where(here, 1.0 / jnp.sqrt(second - average * average + EPSILON), 0.0)

    def everywhere(row):
        return row + pltpu.roll(row, 64, 1) + pltpu.roll(row, 96, 1)

    spread_all = everywhere(spread)
    unit = spread_all * (cross - everywhere(average) * column_totals)
    lane1 = lax.broadcasted_iota(jnp.int32, (1, 128), 1)
    z, y, c, x = (lax.axis_index(name) for name in "zycx")
    tile = 32 * x + 8 * y + 4 * c + lax.shift_right_logical(z, 2)
    comps = comp_ref[...]
    comp = jnp.sum(jnp.where(lane1 == tile, comps, 0), axis=1, keepdims=True)
    size = 128.0 * jnp.sum((comps == comp).astype(F32), axis=1, keepdims=True)
    inverse = 1.0 / size
    coefficients = spread_all * unit * inverse
    pheno_unit = jnp.where(here, unit[PHENO - 48 : PHENO - 47], 0.0)
    energy = jnp.sum(pheno_unit * pheno_unit * inverse, axis=1, keepdims=True)
    parts = three_parts(average)
    row = lax.broadcasted_iota(jnp.int32, (24, 128), 0)
    group = lane_group((24, 128))
    last = jnp.where(row < 16, coefficients, stacked([average] * 16 + list(parts), 24))
    packed = jnp.where(group == 2, last, jnp.where(group < 2, coefficients, 0.0)).astype(BF16)
    for d in range(16):
        coef_ref[d] = packed
    weight_all = jnp.sum(jnp.where(lane1 == 64, weight, 0.0), axis=1, keepdims=True)
    extra_ref[...] = stacked(
        [
            jnp.where(lane1 == 64 + comp, energy, 0.0),
            jnp.broadcast_to(weight_all, (1, 128)),
        ],
        8,
    )


def unpack_kernel(in_ref, out_ref):
    group = lane_group((24, 128))
    for tile in range(4):
        blocks = [in_ref[4 * tile + q].astype(F32) for q in range(4)]
        rows = []
        for k in range(3):
            row = None
            for q in range(4):
                shift = (32 * (q - k)) % 128
                moved = pltpu.roll(blocks[q], shift, 1) if shift else blocks[q]
                row = moved if row is None else jnp.where(group == q, moved, row)
            rows.append(row)
        whole = jnp.concatenate(rows, axis=0).astype(BF16)
        for d in range(4):
            out_ref[d, :, 128 * tile : 128 * tile + 128] = whole


def images_kernel(comp_ref, words_ref, root_ref, coef_ref, out_ref, acc_ref):
    acc_ref[...] = jnp.zeros_like(acc_ref)
    words = words_ref[...]
    lane = lax.broadcasted_iota(jnp.int32, (264, 128), 1)
    blank = jnp.zeros((PROBES, 128), BF16)
    for tile in range(0, 32, 2):
        y, c = divmod(tile // 4, 2)
        at = 128 * (tile % 4)
        weights = coef_ref[c, y, :PROBES, at : at + 256]
        averages = coef_ref[c, y, PROBES:, at : at + 256].astype(F32)
        x = jnp.concatenate([dosage_tile(words, tile), dosage_tile(words, tile + 1)], axis=1)
        x = jnp.concatenate([x, averages], axis=0).astype(BF16)
        left = jnp.concatenate([weights[:, :128], blank], axis=1)
        right = jnp.concatenate([blank, weights[:, 128:]], axis=1)
        product = dot_nt(x, jnp.concatenate([left, right], axis=0))
        comp = comp_ref[tile]
        acc_ref[comp] = acc_ref[comp] + jnp.where(lane < PROBES, product, 0.0)
        comp = comp_ref[tile + 1]
        acc_ref[comp] = acc_ref[comp] + jnp.where(lane < PROBES, 0.0, product)
    column = jnp.broadcast_to(root_ref[...], (128, root_ref.shape[1])).T
    for pair in range(4):
        halves = []
        for k in (2 * pair, 2 * pair + 1):
            total = acc_ref[k]
            total = total + pltpu.roll(total, PROBES, 1)
            centre = total[256:257] + total[257:258] + total[258:259]
            halves.append(total[:256] - centre)
        out_ref[:, 128 * pair : 128 * pair + 128] = (
            jnp.where(lane[:256] < PROBES, *halves) * column
        ).astype(BF16)


def trace_places():
    low, high = np.zeros((24, 128), np.float32), np.zeros((24, 128), np.float32)
    r = 0
    for turned in (0, 1):
        for a in range(4):
            for b in range(a, 4):
                for table, k, l in (
                    (low, 2 * a, 2 * b + turned),
                    (high, 2 * a + 1, 2 * b + 1 - turned),
                ):
                    if turned and a == b and table is high:
                        continue
                    table[r, 8 * k + l] = 1.0
                    table[r, 8 * l + k] = 1.0
                r += 1
    return low, high


def trace_kernel(in_ref, extra_ref, low_ref, high_ref, images_ref, sums_ref):
    full = in_ref[0].astype(F32)
    for d in range(1, 4):
        full = full + in_ref[d].astype(F32)
    images_ref[...] = full.astype(BF16)
    tiles = [full[:, 128 * a : 128 * a + 128] for a in range(4)]
    turned = [pltpu.roll(t, 64, 1) for t in tiles]
    rows = []
    for others in (tiles, turned):
        for a in range(4):
            for b in range(a, 4):
                rows.append(jnp.sum(tiles[a] * others[b], axis=0, keepdims=True))
    products = stacked(rows, 24)
    lane = lax.broadcasted_iota(jnp.int32, products.shape, 1)
    low = jnp.sum(jnp.where(lane < 64, products, 0.0), axis=1, keepdims=True)
    high = jnp.sum(jnp.where(lane < 64, 0.0, products), axis=1, keepdims=True)
    sums = jnp.sum(low * low_ref[...] + high * high_ref[...], axis=0, keepdims=True)
    sums = sums + extra_ref[0:1]
    sums_ref[...] = jnp.broadcast_to(sums[None], sums_ref.shape)


def middle_kernel(in_ref, out_ref):
    out_ref[...] = jnp.broadcast_to(jnp.sum(in_ref[...], axis=0, keepdims=True), out_ref.shape)


def last_kernel(in_ref, extra_ref, held_ref, images_ref, traces_ref, yky_ref):
    images_ref[...] = held_ref[...]
    sums = jnp.sum(in_ref[...], axis=0)
    weight = extra_ref[1:2]
    scaled = sums * (SNPS / (COMPS * PROBES)) / (weight * weight)
    rows = [scaled] + [pltpu.roll(scaled, 128 - 8 * k, 1) for k in range(1, 8)]
    traces_ref[...] = stacked(rows, 8)[:, :8]
    yky_ref[...] = pltpu.roll(sums / weight, 64, 1)[:, :8]


def call(kernel, out, scalars=0, **kwargs):
    def run(*args):
        specs = [pl.BlockSpec(memory_space=pltpu.SMEM)] * scalars
        specs += [pl.BlockSpec(memory_space=pltpu.VMEM)] * (len(args) - scalars)
        return pl.pallas_call(kernel, out_shape=out, in_specs=specs, **kwargs)(*args)

    return run


def near(array):
    return pltpu.with_memory_space_constraint(array, pltpu.VMEM)


def shape(dims, dtype):
    return jax.ShapeDtypeStruct(dims, dtype)


def on_device(geno_words, counts, probes, phenotype, tile_comp):
    comp_row = tile_comp.reshape(1, -1)
    sent, root, comps, own_comps = call(
        panel_kernel,
        [
            pltpu.VMEM((8, ROWS, 512), BF16),
            pltpu.VMEM((1, 256), F32),
            pltpu.VMEM((1, 128), jnp.int32),
            pltpu.SMEM((32,), jnp.int32),
        ],
        scalars=1,
        out_specs=[pl.BlockSpec(memory_space=pltpu.VMEM)] * 3
        + [pl.BlockSpec(memory_space=pltpu.SMEM)],
    )(
        tile_comp,
        geno_words,
        probes.T,
        counts.reshape(1, -1),
        phenotype.reshape(1, -1),
        comp_row,
    )
    got = lax.all_to_all(sent, ("y", "c"), 0, 0, tiled=True)
    sent = call(regroup_kernel, pltpu.VMEM((16, 24, 128), BF16))(near(got))
    got = lax.all_to_all(sent, "z", 0, 0, tiled=True)
    sent, extra = call(
        finish_kernel, (pltpu.VMEM((16, 24, 128), BF16), pltpu.VMEM((8, 128), F32))
    )(near(comps), near(got))
    got = lax.all_to_all(sent, "z", 0, 0, tiled=True)
    sent = call(unpack_kernel, pltpu.VMEM((4, ROWS, 512), BF16))(near(got))
    got = lax.all_to_all(sent, "y", 0, 0, tiled=True)
    coefficients = lax.all_gather(got, "c")
    partial = call(
        images_kernel,
        pltpu.VMEM((256, COMPS * PROBES), BF16),
        scalars=1,
        scratch_shapes=[pltpu.VMEM((COMPS, 264, 128), F32)],
    )(
        pltpu.with_memory_space_constraint(own_comps, pltpu.SMEM),
        near(geno_words),
        near(root),
        near(coefficients),
    )
    pieces = lax.all_to_all(partial.reshape(4, 64, COMPS * PROBES), "x", 0, 0, tiled=True)
    low, high = trace_places()
    images, sums = call(
        trace_kernel, (pltpu.VMEM((64, COMPS * PROBES), BF16), pltpu.VMEM((16, 1, 128), F32))
    )(near(pieces), near(extra), near(jnp.asarray(low)), near(jnp.asarray(high)))
    got = lax.all_to_all(sums, "z", 0, 0, tiled=True)
    sums = call(middle_kernel, pltpu.VMEM((32, 1, 128), F32))(near(got))
    got = lax.all_to_all(sums, ("y", "c", "x"), 0, 0, tiled=True)
    images, traces, yky = call(
        last_kernel,
        (shape((64, COMPS * PROBES), BF16), shape((8, 8), F32), shape((1, 8), F32)),
    )(near(got), near(extra), near(images))
    return images, traces, yky.reshape(8)


def solution(mesh):
    split = Mesh(mesh.devices.reshape(16, 4, 2, 4), ("z", "y", "c", "x"))
    samples = ("z", "y", "c")
    return jax.shard_map(
        on_device,
        mesh=split,
        in_specs=(P(samples, "x"), P(samples), P(samples, None), P(samples), P()),
        out_specs=(P((*samples, "x"), None), P(), P()),
        check_vma=False,
    )
```

```python
import jax
import jax.numpy as jnp
import numpy as np
from jax import lax
from jax.experimental import pallas as pl
from jax.experimental.pallas import tpu as pltpu
from jax.sharding import Mesh
from jax.sharding import PartitionSpec as P

SNPS = 16384
COMPS = 8
PROBES = 64
EPSILON = 1e-05
F32 = jnp.float32
BF16 = jnp.bfloat16

PHENO, FIRST, SQUARE, RATE, TOTALS = 64, 65, 67, 69, 70
COUNT = 65
ROWS = 72


def rounded(v):
    return v.astype(BF16).astype(F32)


def two_parts(v):
    high = rounded(v)
    return high, v - high


def three_parts(v):
    high = rounded(v)
    rest = v - high
    mid = rounded(rest)
    return high, mid, rest - mid


def stacked(rows, height):
    width = rows[0].shape[1]
    at = lax.broadcasted_iota(jnp.int32, (height, width), 0)
    out = jnp.zeros((height, width), F32)
    for i, row in enumerate(rows):
        out = jnp.where(at == i, jnp.broadcast_to(row, (height, width)), out)
    return out


def rate_of(weight):
    return rounded(1.0 / jnp.maximum(weight, 1.0))


def dot_tn(a, b):
    return lax.dot_general(a, b, (((0,), (0,)), ((), ())), preferred_element_type=F32)


def dot_nt(a, b):
    return lax.dot_general(a, b, (((1,), (1,)), ((), ())), preferred_element_type=F32)


def dosage_tile(words, tile):
    half, field = divmod(tile, 16)
    block = words[:, 128 * half : 128 * half + 128]
    return (lax.shift_right_logical(block, jnp.int32(2 * field)) & 3).astype(F32)


def panel_kernel(
    comp_ref, words_ref, probes_ref, counts_ref, pheno_ref, comps_ref, out_ref, root_ref, held_ref, own_ref
):
    held_ref[...] = comps_ref[...]
    first_tile = 32 * lax.axis_index("x")
    for tile in range(32):
        own_ref[tile] = comp_ref[first_tile + tile]
    counts = counts_ref[...].astype(F32)
    root = jnp.sqrt(counts)
    root_ref[...] = root
    probe_rows = rounded(probes_ref[...].astype(F32) * root)
    pheno_rows = rounded(pheno_ref[...] * root)
    tail = stacked([pheno_rows, counts], 64)
    left_all = jnp.concatenate([probe_rows, tail], axis=0)
    left = left_all[:ROWS].astype(BF16)
    left_tail = left_all[64:72].astype(BF16)
    totals = dot_nt(jnp.ones((8, left_all.shape[1]), BF16), left_all.astype(BF16))[:1]
    column = jnp.sum(left_all[:ROWS], axis=1, keepdims=True)
    rate = rate_of(jnp.sum(counts, axis=1, keepdims=True))
    parts = three_parts(totals)
    totals_row = jnp.concatenate([*parts, jnp.zeros_like(totals)], axis=1)
    words = words_ref[...]
    for group in range(8):
        x = jnp.concatenate([dosage_tile(words, 4 * group + i) for i in range(4)], axis=1)
        x = x.astype(BF16)
        sums = jnp.dot(left, x, preferred_element_type=F32)
        squares = jnp.dot(left_tail, x * x, preferred_element_type=F32)[1:2]
        first = sums[COUNT : COUNT + 1]
        centre = rounded(first * rate)
        centred = sums - column * centre
        lower = stacked(
            [
                centred[PHENO : PHENO + 1],
                *two_parts(first),
                *two_parts(squares),
                jnp.broadcast_to(rate, first.shape),
                totals_row,
            ],
            8,
        )
        out_ref[group] = jnp.concatenate([centred[:64], lower], axis=0).astype(BF16)


def lane_group(shape):
    return lax.broadcasted_iota(jnp.int32, shape, 1) // 32


def regroup_kernel(in_ref, out_ref):
    total = jnp.zeros((ROWS, 512), F32)
    centres, parts = [], [[], [], []]
    for d in range(8):
        block = in_ref[d].astype(F32)
        total = total + block
        first = block[FIRST : FIRST + 1] + block[FIRST + 1 : FIRST + 2]
        centres.append(first * block[RATE : RATE + 1])
        for s in range(3):
            parts[s].append(block[TOTALS : TOTALS + 1, 128 * s : 128 * s + 128])
    centre8 = stacked(centres, 8)
    left = jnp.concatenate([stacked(rows, 8) for rows in parts], axis=0)
    totals = jnp.sum(left, axis=0, keepdims=True)
    lane = lax.broadcasted_iota(jnp.int32, totals.shape, 1)
    weight = jnp.sum(jnp.where(lane == COUNT, totals, 0.0), axis=1, keepdims=True)
    rate = rate_of(weight)
    first = total[FIRST : FIRST + 1] + total[FIRST + 1 : FIRST + 2]
    squares = total[SQUARE : SQUARE + 1] + total[SQUARE + 1 : SQUARE + 2]
    centre = jnp.broadcast_to(first * rate, (8, 512))
    right = jnp.concatenate([centre8] * 3 + [centre] * 3, axis=0).astype(BF16)
    left = jnp.concatenate([left, -left], axis=0).astype(BF16)
    centred = total + dot_tn(left, right)[:ROWS]
    lower = stacked(
        [
            centred[PHENO : PHENO + 1],
            *two_parts(first),
            *two_parts(squares),
            jnp.broadcast_to(rate, first.shape),
        ],
        8,
    )
    full = jnp.concatenate([centred[:64], lower], axis=0)
    rows = []
    for part in three_parts(totals):
        for k in range(3):
            rows.append(pltpu.roll(part, (96 - 24 * k) % 128, 1) if 96 - 24 * k else part)
    totals_block = stacked(rows, 24)
    group = lane_group((24, 128))
    for tile in range(4):
        blocks = [full[24 * k : 24 * k + 24, 128 * tile : 128 * tile + 128] for k in range(3)]
        for q in range(4):
            packed = totals_block
            for k in range(3):
                shift = (32 * (k - q)) % 128
                moved = pltpu.roll(blocks[k], shift, 1) if shift else blocks[k]
                packed = jnp.where(group == k, moved, packed)
            out_ref[4 * tile + q] = packed.astype(BF16)


def finish_kernel(comp_ref, in_ref, coef_ref, extra_ref):
    total = jnp.zeros((24, 128), F32)
    group16 = lane_group((16, 128))
    lane16 = lax.broadcasted_iota(jnp.int32, (16, 128), 1)
    centres, parts = [], [[] for _ in range(9)]
    for d in range(16):
        block = in_ref[d].astype(F32)
        total = total + block
        first = block[FIRST - 48 : FIRST - 47] + block[FIRST - 47 : FIRST - 46]
        centres.append(first * block[RATE - 48 : RATE - 47])
        for i in range(9):
            parts[i].append(block[i : i + 1])
    centre16 = jnp.where(group16 == 2, rounded(stacked(centres, 16)), 0.0)
    kept = (lane16 >= 96) & (lane16 < 120)
    left = jnp.concatenate([jnp.where(kept, stacked(rows, 16), 0.0) for rows in parts], axis=0)
    moved = [pltpu.roll(centre16, 64, 1), pltpu.roll(centre16, 96, 1), centre16]
    marks = [(group16 == k).astype(F32) for k in range(3)]
    right = jnp.concatenate(
        [jnp.concatenate(moved * 3, axis=0), jnp.concatenate(marks * 3, axis=0)], axis=1
    )
    outer = dot_tn(left.astype(BF16), right.astype(BF16))[96:120]
    cross = total + outer[:, :128]
    column_totals = outer[:, 128:]
    group1 = lane_group((1, 128))
    here = group1 == 2
    weight = column_totals[COUNT - 48 : COUNT - 47]
    weight = jnp.where(here, weight, 1.0)
    first = total[FIRST - 48 : FIRST - 47] + total[FIRST - 47 : FIRST - 46]
    squares = total[SQUARE - 48 : SQUARE - 47] + total[SQUARE - 47 : SQUARE - 46]
    average = jnp.where(here, first / weight, 0.0)
    second = jnp.where(here, squares / weight, 0.0)
    spread = jnp.where(here, 1.0 / jnp.sqrt(second - average * average + EPSILON), 0.0)

    def everywhere(row):
        return row + pltpu.roll(row, 64, 1) + pltpu.roll(row, 96, 1)

    spread_all = everywhere(spread)
    unit = spread_all * (cross - everywhere(average) * column_totals)
    lane1 = lax.broadcasted_iota(jnp.int32, (1, 128), 1)
    z, y, c, x = (lax.axis_index(name) for name in "zycx")
    tile = 32 * x + 8 * y + 4 * c + lax.shift_right_logical(z, 2)
    comps = comp_ref[...]
    comp = jnp.sum(jnp.where(lane1 == tile, comps, 0), axis=1, keepdims=True)
    size = 128.0 * jnp.sum((comps == comp).astype(F32), axis=1, keepdims=True)
    inverse = 1.0 / size
    coefficients = spread_all * unit * inverse
    pheno_unit = jnp.where(here, unit[PHENO - 48 : PHENO - 47], 0.0)
    energy = jnp.sum(pheno_unit * pheno_unit * inverse, axis=1, keepdims=True)
    parts = three_parts(average)
    row = lax.broadcasted_iota(jnp.int32, (24, 128), 0)
    group = lane_group((24, 128))
    last = jnp.where(row < 16, coefficients, stacked([average] * 16 + list(parts), 24))
    packed = jnp.where(group == 2, last, jnp.where(group < 2, coefficients, 0.0)).astype(BF16)
    for d in range(16):
        coef_ref[d] = packed
    weight_all = jnp.sum(jnp.where(lane1 == 64, weight, 0.0), axis=1, keepdims=True)
    extra_ref[...] = stacked(
        [
            jnp.where(lane1 == 64 + comp, energy, 0.0),
            jnp.broadcast_to(weight_all, (1, 128)),
        ],
        8,
    )


def unpack_kernel(in_ref, out_ref):
    group = lane_group((24, 128))
    for tile in range(4):
        blocks = [in_ref[4 * tile + q].astype(F32) for q in range(4)]
        rows = []
        for k in range(3):
            row = None
            for q in range(4):
                shift = (32 * (q - k)) % 128
                moved = pltpu.roll(blocks[q], shift, 1) if shift else blocks[q]
                row = moved if row is None else jnp.where(group == q, moved, row)
            rows.append(row)
        whole = jnp.concatenate(rows, axis=0).astype(BF16)
        for d in range(4):
            out_ref[d, :, 128 * tile : 128 * tile + 128] = whole


def images_kernel(comp_ref, words_ref, root_ref, coef_ref, out_ref, acc_ref):
    acc_ref[...] = jnp.zeros_like(acc_ref)
    words = words_ref[...]
    lane = lax.broadcasted_iota(jnp.int32, (264, 128), 1)
    blank = jnp.zeros((PROBES, 128), BF16)
    for tile in range(0, 32, 2):
        y, c = divmod(tile // 4, 2)
        at = 128 * (tile % 4)
        weights = coef_ref[c, y, :PROBES, at : at + 256]
        averages = coef_ref[c, y, PROBES:, at : at + 256].astype(F32)
        x = jnp.concatenate([dosage_tile(words, tile), dosage_tile(words, tile + 1)], axis=1)
        x = jnp.concatenate([x, averages], axis=0).astype(BF16)
        left = jnp.concatenate([weights[:, :128], blank], axis=1)
        right = jnp.concatenate([blank, weights[:, 128:]], axis=1)
        product = dot_nt(x, jnp.concatenate([left, right], axis=0))
        comp = comp_ref[tile]
        acc_ref[comp] = acc_ref[comp] + jnp.where(lane < PROBES, product, 0.0)
        comp = comp_ref[tile + 1]
        acc_ref[comp] = acc_ref[comp] + jnp.where(lane < PROBES, 0.0, product)
    column = jnp.broadcast_to(root_ref[...], (128, root_ref.shape[1])).T
    for pair in range(4):
        halves = []
        for k in (2 * pair, 2 * pair + 1):
            total = acc_ref[k]
            total = total + pltpu.roll(total, PROBES, 1)
            centre = total[256:257] + total[257:258] + total[258:259]
            halves.append(total[:256] - centre)
        out_ref[:, 128 * pair : 128 * pair + 128] = (
            jnp.where(lane[:256] < PROBES, *halves) * column
        ).astype(BF16)


def trace_places():
    low, high = np.zeros((24, 128), np.float32), np.zeros((24, 128), np.float32)
    r = 0
    for turned in (0, 1):
        for a in range(4):
            for b in range(a, 4):
                for table, k, l in (
                    (low, 2 * a, 2 * b + turned),
                    (high, 2 * a + 1, 2 * b + 1 - turned),
                ):
                    if turned and a == b and table is high:
                        continue
                    table[r, 8 * k + l] = 1.0
                    table[r, 8 * l + k] = 1.0
                r += 1
    return low, high


def trace_kernel(in_ref, extra_ref, low_ref, high_ref, images_ref, sums_ref):
    full = in_ref[0].astype(F32)
    for d in range(1, 4):
        full = full + in_ref[d].astype(F32)
    images_ref[...] = full.astype(BF16)
    tiles = [full[:, 128 * a : 128 * a + 128] for a in range(4)]
    turned = [pltpu.roll(t, 64, 1) for t in tiles]
    rows = []
    for others in (tiles, turned):
        for a in range(4):
            for b in range(a, 4):
                rows.append(jnp.sum(tiles[a] * others[b], axis=0, keepdims=True))
    products = stacked(rows, 24)
    lane = lax.broadcasted_iota(jnp.int32, products.shape, 1)
    low = jnp.sum(jnp.where(lane < 64, products, 0.0), axis=1, keepdims=True)
    high = jnp.sum(jnp.where(lane < 64, 0.0, products), axis=1, keepdims=True)
    sums = jnp.sum(low * low_ref[...] + high * high_ref[...], axis=0, keepdims=True)
    sums = sums + extra_ref[0:1]
    sums_ref[...] = jnp.broadcast_to(sums[None], sums_ref.shape)


def middle_kernel(in_ref, out_ref):
    out_ref[...] = jnp.broadcast_to(jnp.sum(in_ref[...], axis=0, keepdims=True), out_ref.shape)


def last_kernel(in_ref, extra_ref, held_ref, images_ref, traces_ref, yky_ref):
    images_ref[...] = held_ref[...]
    sums = jnp.sum(in_ref[...], axis=0)
    weight = extra_ref[1:2]
    scaled = sums * (SNPS / (COMPS * PROBES)) / (weight * weight)
    rows = [scaled] + [pltpu.roll(scaled, 128 - 8 * k, 1) for k in range(1, 8)]
    traces_ref[...] = stacked(rows, 8)[:, :8]
    yky_ref[...] = pltpu.roll(sums / weight, 64, 1)[:, :8]


def call(kernel, out, scalars=0, **kwargs):
    def run(*args):
        specs = [pl.BlockSpec(memory_space=pltpu.SMEM)] * scalars
        specs += [pl.BlockSpec(memory_space=pltpu.VMEM)] * (len(args) - scalars)
        return pl.pallas_call(kernel, out_shape=out, in_specs=specs, **kwargs)(*args)

    return run


def near(array):
    return pltpu.with_memory_space_constraint(array, pltpu.VMEM)


def shape(dims, dtype):
    return jax.ShapeDtypeStruct(dims, dtype)


def on_device(geno_words, counts, probes, phenotype, tile_comp):
    comp_row = tile_comp.reshape(1, -1)
    sent, root, comps, own_comps = call(
        panel_kernel,
        [
            pltpu.VMEM((8, ROWS, 512), BF16),
            pltpu.VMEM((1, 256), F32),
            pltpu.VMEM((1, 128), jnp.int32),
            pltpu.SMEM((32,), jnp.int32),
        ],
        scalars=1,
        out_specs=[pl.BlockSpec(memory_space=pltpu.VMEM)] * 3
        + [pl.BlockSpec(memory_space=pltpu.SMEM)],
    )(
        tile_comp,
        geno_words,
        probes.T,
        counts.reshape(1, -1),
        phenotype.reshape(1, -1),
        comp_row,
    )
    got = lax.all_to_all(sent, ("y", "c"), 0, 0, tiled=True)
    sent = call(regroup_kernel, pltpu.VMEM((16, 24, 128), BF16))(near(got))
    got = lax.all_to_all(sent, "z", 0, 0, tiled=True)
    sent, extra = call(
        finish_kernel, (pltpu.VMEM((16, 24, 128), BF16), pltpu.VMEM((8, 128), F32))
    )(near(comps), near(got))
    got = lax.all_to_all(sent, "z", 0, 0, tiled=True)
    sent = call(unpack_kernel, pltpu.VMEM((4, ROWS, 512), BF16))(near(got))
    got = lax.all_to_all(sent, "y", 0, 0, tiled=True)
    coefficients = lax.all_gather(got, "c")
    partial = call(
        images_kernel,
        pltpu.VMEM((256, COMPS * PROBES), BF16),
        scalars=1,
        scratch_shapes=[pltpu.VMEM((COMPS, 264, 128), F32)],
    )(
        pltpu.with_memory_space_constraint(own_comps, pltpu.SMEM),
        near(geno_words),
        near(root),
        near(coefficients),
    )
    pieces = lax.all_to_all(partial.reshape(4, 64, COMPS * PROBES), "x", 0, 0, tiled=True)
    low, high = trace_places()
    images, sums = call(
        trace_kernel, (pltpu.VMEM((64, COMPS * PROBES), BF16), pltpu.VMEM((32, 1, 128), F32))
    )(near(pieces), near(extra), near(jnp.asarray(low)), near(jnp.asarray(high)))
    got = lax.all_to_all(sums, ("y", "c", "x"), 0, 0, tiled=True)
    sums = call(middle_kernel, pltpu.VMEM((16, 1, 128), F32))(near(got))
    got = lax.all_to_all(sums, "z", 0, 0, tiled=True)
    images, traces, yky = call(
        last_kernel,
        (shape((64, COMPS * PROBES), BF16), shape((8, 8), F32), shape((1, 8), F32)),
    )(near(got), near(extra), near(images))
    return images, traces, yky.reshape(8)


def solution(mesh):
    split = Mesh(mesh.devices.reshape(16, 4, 2, 4), ("z", "y", "c", "x"))
    samples = ("z", "y", "c")
    return jax.shard_map(
        on_device,
        mesh=split,
        in_specs=(P(samples, "x"), P(samples), P(samples, None), P(samples), P()),
        out_specs=(P((*samples, "x"), None), P(), P()),
        check_vma=False,
    )
```

```python
import jax
import jax.numpy as jnp
import numpy as np
from jax import lax
from jax.experimental import pallas as pl
from jax.experimental.pallas import tpu as pltpu
from jax.sharding import Mesh
from jax.sharding import PartitionSpec as P

SNPS = 16384
COMPS = 8
PROBES = 64
EPSILON = 1e-05
F32 = jnp.float32
BF16 = jnp.bfloat16

PHENO, FIRST, SQUARE, RATE, TOTALS = 64, 65, 67, 69, 70
COUNT = 65
ROWS = 72


def rounded(v):
    return v.astype(BF16).astype(F32)


def two_parts(v):
    high = rounded(v)
    return high, v - high


def three_parts(v):
    high = rounded(v)
    rest = v - high
    mid = rounded(rest)
    return high, mid, rest - mid


def stacked(rows, height):
    width = rows[0].shape[1]
    at = lax.broadcasted_iota(jnp.int32, (height, width), 0)
    out = jnp.zeros((height, width), F32)
    for i, row in enumerate(rows):
        out = jnp.where(at == i, jnp.broadcast_to(row, (height, width)), out)
    return out


def rate_of(weight):
    return rounded(1.0 / jnp.maximum(weight, 1.0))


def dot_tn(a, b):
    return lax.dot_general(a, b, (((0,), (0,)), ((), ())), preferred_element_type=F32)


def dot_nt(a, b):
    return lax.dot_general(a, b, (((1,), (1,)), ((), ())), preferred_element_type=F32)


def dosage_tile(words, tile):
    half, field = divmod(tile, 16)
    block = words[:, 128 * half : 128 * half + 128]
    return (lax.shift_right_logical(block, jnp.int32(2 * field)) & 3).astype(F32)


def panel_kernel(
    comp_ref, words_ref, probes_ref, counts_ref, pheno_ref, comps_ref, out_ref, root_ref, held_ref, own_ref
):
    held_ref[...] = comps_ref[...]
    first_tile = 32 * lax.axis_index("x")
    for tile in range(32):
        own_ref[tile] = comp_ref[first_tile + tile]
    counts = counts_ref[...].astype(F32)
    root = jnp.sqrt(counts)
    root_ref[...] = root
    probe_rows = rounded(probes_ref[...].astype(F32) * root)
    pheno_rows = rounded(pheno_ref[...] * root)
    tail = stacked([pheno_rows, counts], 64)
    left_all = jnp.concatenate([probe_rows, tail], axis=0)
    left = left_all[:ROWS].astype(BF16)
    left_tail = left_all[64:72].astype(BF16)
    totals = dot_nt(jnp.ones((8, left_all.shape[1]), BF16), left_all.astype(BF16))[:1]
    column = jnp.sum(left_all[:ROWS], axis=1, keepdims=True)
    rate = rate_of(jnp.sum(counts, axis=1, keepdims=True))
    parts = three_parts(totals)
    totals_row = jnp.concatenate([*parts, jnp.zeros_like(totals)], axis=1)
    words = words_ref[...]
    for group in range(8):
        x = jnp.concatenate([dosage_tile(words, 4 * group + i) for i in range(4)], axis=1)
        x = x.astype(BF16)
        sums = jnp.dot(left, x, preferred_element_type=F32)
        squares = jnp.dot(left_tail, x * x, preferred_element_type=F32)[1:2]
        first = sums[COUNT : COUNT + 1]
        centre = rounded(first * rate)
        centred = sums - column * centre
        lower = stacked(
            [
                centred[PHENO : PHENO + 1],
                *two_parts(first),
                *two_parts(squares),
                jnp.broadcast_to(rate, first.shape),
                totals_row,
            ],
            8,
        )
        out_ref[group] = jnp.concatenate([centred[:64], lower], axis=0).astype(BF16)


def lane_group(shape):
    return lax.broadcasted_iota(jnp.int32, shape, 1) // 32


def regroup_kernel(in_ref, out_ref):
    total = jnp.zeros((ROWS, 512), F32)
    centres, parts = [], [[], [], []]
    for d in range(8):
        block = in_ref[d].astype(F32)
        total = total + block
        first = block[FIRST : FIRST + 1] + block[FIRST + 1 : FIRST + 2]
        centres.append(first * block[RATE : RATE + 1])
        for s in range(3):
            parts[s].append(block[TOTALS : TOTALS + 1, 128 * s : 128 * s + 128])
    centre8 = stacked(centres, 8)
    left = jnp.concatenate([stacked(rows, 8) for rows in parts], axis=0)
    totals = jnp.sum(left, axis=0, keepdims=True)
    lane = lax.broadcasted_iota(jnp.int32, totals.shape, 1)
    weight = jnp.sum(jnp.where(lane == COUNT, totals, 0.0), axis=1, keepdims=True)
    rate = rate_of(weight)
    first = total[FIRST : FIRST + 1] + total[FIRST + 1 : FIRST + 2]
    squares = total[SQUARE : SQUARE + 1] + total[SQUARE + 1 : SQUARE + 2]
    centre = jnp.broadcast_to(first * rate, (8, 512))
    right = jnp.concatenate([centre8] * 3 + [centre] * 3, axis=0).astype(BF16)
    left = jnp.concatenate([left, -left], axis=0).astype(BF16)
    centred = total + dot_tn(left, right)[:ROWS]
    lower = stacked(
        [
            centred[PHENO : PHENO + 1],
            *two_parts(first),
            *two_parts(squares),
            jnp.broadcast_to(rate, first.shape),
        ],
        8,
    )
    full = jnp.concatenate([centred[:64], lower], axis=0)
    rows = []
    for part in three_parts(totals):
        for k in range(3):
            rows.append(pltpu.roll(part, (96 - 24 * k) % 128, 1) if 96 - 24 * k else part)
    totals_block = stacked(rows, 24)
    group = lane_group((24, 128))
    for tile in range(4):
        blocks = [full[24 * k : 24 * k + 24, 128 * tile : 128 * tile + 128] for k in range(3)]
        for q in range(4):
            packed = totals_block
            for k in range(3):
                shift = (32 * (k - q)) % 128
                moved = pltpu.roll(blocks[k], shift, 1) if shift else blocks[k]
                packed = jnp.where(group == k, moved, packed)
            out_ref[4 * tile + q] = packed.astype(BF16)


def finish_kernel(comp_ref, in_ref, coef_ref, extra_ref):
    total = jnp.zeros((24, 128), F32)
    group16 = lane_group((16, 128))
    lane16 = lax.broadcasted_iota(jnp.int32, (16, 128), 1)
    centres, parts = [], [[] for _ in range(9)]
    for d in range(16):
        block = in_ref[d].astype(F32)
        total = total + block
        first = block[FIRST - 48 : FIRST - 47] + block[FIRST - 47 : FIRST - 46]
        centres.append(first * block[RATE - 48 : RATE - 47])
        for i in range(9):
            parts[i].append(block[i : i + 1])
    centre16 = jnp.where(group16 == 2, rounded(stacked(centres, 16)), 0.0)
    kept = (lane16 >= 96) & (lane16 < 120)
    left = jnp.concatenate([jnp.where(kept, stacked(rows, 16), 0.0) for rows in parts], axis=0)
    moved = [pltpu.roll(centre16, 64, 1), pltpu.roll(centre16, 96, 1), centre16]
    marks = [(group16 == k).astype(F32) for k in range(3)]
    right = jnp.concatenate(
        [jnp.concatenate(moved * 3, axis=0), jnp.concatenate(marks * 3, axis=0)], axis=1
    )
    outer = dot_tn(left.astype(BF16), right.astype(BF16))[96:120]
    cross = total + outer[:, :128]
    column_totals = outer[:, 128:]
    group1 = lane_group((1, 128))
    here = group1 == 2
    weight = column_totals[COUNT - 48 : COUNT - 47]
    weight = jnp.where(here, weight, 1.0)
    first = total[FIRST - 48 : FIRST - 47] + total[FIRST - 47 : FIRST - 46]
    squares = total[SQUARE - 48 : SQUARE - 47] + total[SQUARE - 47 : SQUARE - 46]
    average = jnp.where(here, first / weight, 0.0)
    second = jnp.where(here, squares / weight, 0.0)
    spread = jnp.where(here, 1.0 / jnp.sqrt(second - average * average + EPSILON), 0.0)

    def everywhere(row):
        return row + pltpu.roll(row, 64, 1) + pltpu.roll(row, 96, 1)

    spread_all = everywhere(spread)
    unit = spread_all * (cross - everywhere(average) * column_totals)
    lane1 = lax.broadcasted_iota(jnp.int32, (1, 128), 1)
    z, y, c, x = (lax.axis_index(name) for name in "zycx")
    tile = 32 * x + 8 * y + 4 * c + lax.shift_right_logical(z, 2)
    comps = comp_ref[...]
    comp = jnp.sum(jnp.where(lane1 == tile, comps, 0), axis=1, keepdims=True)
    size = 128.0 * jnp.sum((comps == comp).astype(F32), axis=1, keepdims=True)
    inverse = 1.0 / size
    coefficients = spread_all * unit * inverse
    pheno_unit = jnp.where(here, unit[PHENO - 48 : PHENO - 47], 0.0)
    energy = jnp.sum(pheno_unit * pheno_unit * inverse, axis=1, keepdims=True)
    parts = three_parts(average)
    row = lax.broadcasted_iota(jnp.int32, (24, 128), 0)
    group = lane_group((24, 128))
    last = jnp.where(row < 16, coefficients, stacked([average] * 16 + list(parts), 24))
    packed = jnp.where(group == 2, last, jnp.where(group < 2, coefficients, 0.0)).astype(BF16)
    for d in range(16):
        coef_ref[d] = packed
    weight_all = jnp.sum(jnp.where(lane1 == 64, weight, 0.0), axis=1, keepdims=True)
    extra_ref[...] = stacked(
        [
            jnp.where(lane1 == 64 + comp, energy, 0.0),
            jnp.broadcast_to(weight_all, (1, 128)),
        ],
        8,
    )


def unpack_kernel(in_ref, out_ref):
    group = lane_group((24, 128))
    for tile in range(4):
        blocks = [in_ref[4 * tile + q].astype(F32) for q in range(4)]
        rows = []
        for k in range(3):
            row = None
            for q in range(4):
                shift = (32 * (q - k)) % 128
                moved = pltpu.roll(blocks[q], shift, 1) if shift else blocks[q]
                row = moved if row is None else jnp.where(group == q, moved, row)
            rows.append(row)
        whole = jnp.concatenate(rows, axis=0).astype(BF16)
        for d in range(4):
            out_ref[d, :, 128 * tile : 128 * tile + 128] = whole


def images_kernel(comp_ref, words_ref, root_ref, coef_ref, out_ref, acc_ref, centre_ref):
    acc_ref[...] = jnp.zeros_like(acc_ref)
    centre_ref[...] = jnp.zeros_like(centre_ref)
    words = words_ref[...]
    blank = jnp.zeros((PROBES, 128), BF16)
    for pair in range(0, 32, 2):
        y, c = divmod(pair // 4, 2)
        at = 128 * (pair % 4)
        weights = coef_ref[c, y, :PROBES, at : at + 256]
        averages = coef_ref[c, y, PROBES:, at : at + 256].astype(F32)
        average = averages[0:1] + averages[1:2] + averages[2:3]
        x = jnp.concatenate([dosage_tile(words, pair), dosage_tile(words, pair + 1)], axis=1)
        left = jnp.concatenate([weights[:, :128], blank], axis=1)
        right = jnp.concatenate([blank, weights[:, 128:]], axis=1)
        product = dot_nt(jnp.concatenate([left, right], axis=0), x.astype(BF16))
        shares = weights.astype(F32) * average
        for i in range(2):
            comp = comp_ref[pair + i]
            acc_ref[comp] = acc_ref[comp] + product[PROBES * i : PROBES * i + PROBES]
            centre_ref[comp] = centre_ref[comp] + shares[:, 128 * i : 128 * i + 128]
    root = root_ref[...]
    for pair in range(4):
        halves = []
        for k in (2 * pair, 2 * pair + 1):
            centre = jnp.sum(centre_ref[k], axis=1, keepdims=True)
            halves.append((acc_ref[k] - centre) * root)
        out_ref[:, 128 * pair : 128 * pair + 128] = jnp.concatenate(halves, axis=0).T.astype(BF16)


def trace_places():
    low, high = np.zeros((24, 128), np.float32), np.zeros((24, 128), np.float32)
    r = 0
    for turned in (0, 1):
        for a in range(4):
            for b in range(a, 4):
                for table, k, l in (
                    (low, 2 * a, 2 * b + turned),
                    (high, 2 * a + 1, 2 * b + 1 - turned),
                ):
                    if turned and a == b and table is high:
                        continue
                    table[r, 8 * k + l] = 1.0
                    table[r, 8 * l + k] = 1.0
                r += 1
    return low, high


def trace_kernel(in_ref, extra_ref, low_ref, high_ref, images_ref, sums_ref):
    full = in_ref[0].astype(F32)
    for d in range(1, 4):
        full = full + in_ref[d].astype(F32)
    images_ref[...] = full.astype(BF16)
    tiles = [full[:, 128 * a : 128 * a + 128] for a in range(4)]
    turned = [pltpu.roll(t, 64, 1) for t in tiles]
    rows = []
    for others in (tiles, turned):
        for a in range(4):
            for b in range(a, 4):
                rows.append(jnp.sum(tiles[a] * others[b], axis=0, keepdims=True))
    products = stacked(rows, 24)
    lane = lax.broadcasted_iota(jnp.int32, products.shape, 1)
    low = jnp.sum(jnp.where(lane < 64, products, 0.0), axis=1, keepdims=True)
    high = jnp.sum(jnp.where(lane < 64, 0.0, products), axis=1, keepdims=True)
    sums = jnp.sum(low * low_ref[...] + high * high_ref[...], axis=0, keepdims=True)
    sums = sums + extra_ref[0:1]
    sums_ref[...] = jnp.broadcast_to(sums[None], sums_ref.shape)


def middle_kernel(in_ref, out_ref):
    out_ref[...] = jnp.broadcast_to(jnp.sum(in_ref[...], axis=0, keepdims=True), out_ref.shape)


def last_kernel(in_ref, extra_ref, held_ref, images_ref, traces_ref, yky_ref):
    images_ref[...] = held_ref[...]
    sums = jnp.sum(in_ref[...], axis=0)
    weight = extra_ref[1:2]
    scaled = sums * (SNPS / (COMPS * PROBES)) / (weight * weight)
    rows = [scaled] + [pltpu.roll(scaled, 128 - 8 * k, 1) for k in range(1, 8)]
    traces_ref[...] = stacked(rows, 8)[:, :8]
    yky_ref[...] = pltpu.roll(sums / weight, 64, 1)[:, :8]


def call(kernel, out, scalars=0, **kwargs):
    def run(*args):
        specs = [pl.BlockSpec(memory_space=pltpu.SMEM)] * scalars
        specs += [pl.BlockSpec(memory_space=pltpu.VMEM)] * (len(args) - scalars)
        return pl.pallas_call(kernel, out_shape=out, in_specs=specs, **kwargs)(*args)

    return run


def near(array):
    return pltpu.with_memory_space_constraint(array, pltpu.VMEM)


def shape(dims, dtype):
    return jax.ShapeDtypeStruct(dims, dtype)


def on_device(geno_words, counts, probes, phenotype, tile_comp):
    comp_row = tile_comp.reshape(1, -1)
    sent, root, comps, own_comps = call(
        panel_kernel,
        [
            pltpu.VMEM((8, ROWS, 512), BF16),
            pltpu.VMEM((1, 256), F32),
            pltpu.VMEM((1, 128), jnp.int32),
            pltpu.SMEM((32,), jnp.int32),
        ],
        scalars=1,
        out_specs=[pl.BlockSpec(memory_space=pltpu.VMEM)] * 3
        + [pl.BlockSpec(memory_space=pltpu.SMEM)],
    )(
        tile_comp,
        geno_words,
        probes.T,
        counts.reshape(1, -1),
        phenotype.reshape(1, -1),
        comp_row,
    )
    got = lax.all_to_all(sent, ("y", "c"), 0, 0, tiled=True)
    sent = call(regroup_kernel, pltpu.VMEM((16, 24, 128), BF16))(near(got))
    got = lax.all_to_all(sent, "z", 0, 0, tiled=True)
    sent, extra = call(
        finish_kernel, (pltpu.VMEM((16, 24, 128), BF16), pltpu.VMEM((8, 128), F32))
    )(near(comps), near(got))
    got = lax.all_to_all(sent, "z", 0, 0, tiled=True)
    sent = call(unpack_kernel, pltpu.VMEM((4, ROWS, 512), BF16))(near(got))
    got = lax.all_to_all(sent, "y", 0, 0, tiled=True)
    coefficients = lax.all_gather(got, "c")
    partial = call(
        images_kernel,
        pltpu.VMEM((256, COMPS * PROBES), BF16),
        scalars=1,
        scratch_shapes=[
            pltpu.VMEM((COMPS, PROBES, 256), F32),
            pltpu.VMEM((COMPS, PROBES, 128), F32),
        ],
    )(
        pltpu.with_memory_space_constraint(own_comps, pltpu.SMEM),
        near(geno_words),
        near(root),
        near(coefficients),
    )
    pieces = lax.all_to_all(partial.reshape(4, 64, COMPS * PROBES), "x", 0, 0, tiled=True)
    low, high = trace_places()
    images, sums = call(
        trace_kernel, (pltpu.VMEM((64, COMPS * PROBES), BF16), pltpu.VMEM((32, 1, 128), F32))
    )(near(pieces), near(extra), near(jnp.asarray(low)), near(jnp.asarray(high)))
    got = lax.all_to_all(sums, ("y", "c", "x"), 0, 0, tiled=True)
    sums = call(middle_kernel, pltpu.VMEM((16, 1, 128), F32))(near(got))
    got = lax.all_to_all(sums, "z", 0, 0, tiled=True)
    images, traces, yky = call(
        last_kernel,
        (shape((64, COMPS * PROBES), BF16), shape((8, 8), F32), shape((1, 8), F32)),
    )(near(got), near(extra), near(images))
    return images, traces, yky.reshape(8)


def solution(mesh):
    split = Mesh(mesh.devices.reshape(16, 4, 2, 4), ("z", "y", "c", "x"))
    samples = ("z", "y", "c")
    return jax.shard_map(
        on_device,
        mesh=split,
        in_specs=(P(samples, "x"), P(samples), P(samples, None), P(samples), P()),
        out_specs=(P((*samples, "x"), None), P(), P()),
        check_vma=False,
    )
```
